32 devices in a mesh: lat: 8 (over z, x), fld: 4 (over y, core).
Axes of the slice: x: 2, y: 2, z: 4, core: 2. Of those that a mesh axis runs over, the one named last changes fastest.
Arguments:
- grid_in: bfloat16 [32, 2560, 2688], P('fld', 'lat'), may hold values from -6 to 6
- legendre: bfloat16 [768, 1280, 768], P(('lat', 'fld')), may hold values from -0.15625 to 0.15625
- wave_slot: int32 [768], replicated, may hold values from 512 to 1279, as said below
- lat_modes: int32 [2560], P('lat'), may hold values from 10 to 1280
- gauss_weight: float32 [1280], replicated, may hold values from 0.5 to 2
- diffusion: float32 [32], replicated, may hold values from 0.5 to 8
Outputs:
- grid_out: float32 [32, 2560, 2688], P('fld', 'lat')
- spectra: float32 [2, 768, 32, 768], P(None, 'lat', 'fld')
The draws below stay inside these ranges and needn't reach their ends.
Inputs may be any that keep to these rules, and one draw needn't show every extreme that they name: `wave_slot`: every wavenumber from 512 to 1279 stands in exactly one slot; slots 2 t and 2 t + 1 hold two wavenumbers that sum to 1791, the smaller one in the even slot.
All inputs are finite; a program needn't handle non-finite values.
Results may differ from the reference program's by a relative error of at most 0.0071.
Values may be sent and summed in bfloat16 or wider, within the bound.
No kernel may reach another device: no remote copies, remote signals or barrier semaphores. Data moves between devices by JAX's collectives and lax.ppermute only.
A program may use at most 256 MiB of HBM per device.

```python
import math
import jax
import jax.numpy as jnp
from jax import lax

LMAX = 1279
NLAT = 2560
NLON = 2688
MW = 768
FIELDS = 32


def draw_wave_slot(key, part):
    pair_count = MW // 2
    shuffled = jax.random.permutation(key, pair_count).astype(jnp.int32)
    low_waves = LMAX + 1 - MW + shuffled
    high_waves = LMAX - shuffled
    return jnp.stack([low_waves, high_waves], 1).reshape(MW).astype(jnp.int32)


def draw_lat_modes(key, part):
    rows_index = jnp.arange(NLAT, dtype=jnp.int32)
    polar_rows = jnp.minimum(rows_index, NLAT - 1 - rows_index)
    jitter = jax.random.randint(key, (NLAT,), 0, 32, dtype=jnp.int32)
    modes_grown = 10 + 2 * polar_rows * (LMAX + 1) // (NLAT // 2) + jitter
    return jnp.minimum(modes_grown, LMAX + 1).astype(jnp.int32)


def block_levels(stream_key, shape, split, smallest, largest):
    loudness, own = 1.0, jax.random.fold_in(stream_key, 6)
    for dim, blocks in split:
        steps = jnp.exp(jax.random.uniform(jax.random.fold_in(own, dim), (blocks,), jnp.float32, smallest / len(split), largest / len(split)))
        loudness = loudness * jnp.repeat(steps, shape[dim] // blocks).reshape([-1 if axis == dim else 1 for axis in range(len(shape))])
    return loudness


def scatter_about(key, shape, scale, bound, cuts=(), kind=jnp.bfloat16):
    result = scale * jax.random.normal(key, shape, jnp.float32)
    if cuts:
        result = result * block_levels(key, shape, cuts, -0.22, 0.18)
    return jnp.clip(result, -bound, bound).astype(kind)


def setup_inputs(seed: int = 0) -> dict:
    streams_of = jax.random.split(jax.random.key(seed), 7)
    grid_in = scatter_about(streams_of[0], (FIELDS, NLAT, NLON), 1.0, 6.0, ((0, 4), (1, 8)))
    legendre = scatter_about(streams_of[1], (MW, NLAT // 2, MW), (NLAT // 2) ** -0.5, 0.15625, ((0, 32),))
    wave_slot = draw_wave_slot(jax.random.fold_in(streams_of[6], 71), 0)
    lat_modes = draw_lat_modes(jax.random.fold_in(streams_of[6], 71), 0)
    gauss_weight = jnp.clip(jnp.exp(jax.random.uniform(streams_of[4], (NLAT // 2,), jnp.float32, math.log(0.5), math.log(2.0))), 0.5, 2.0)
    diffusion = jnp.clip(jnp.exp(jax.random.uniform(streams_of[5], (FIELDS,), jnp.float32, math.log(0.5), math.log(8.0))), 0.5, 8.0)
    return {"grid_in": grid_in, "legendre": legendre, "wave_slot": wave_slot, "lat_modes": lat_modes, "gauss_weight": gauss_weight, "diffusion": diffusion}


def angle_table(waves, lon_count):
    points = jnp.arange(lon_count, dtype=jnp.int32)
    phase_index = points[:, None] * waves[None, :] % lon_count
    radians = phase_index.astype(jnp.float32) * (2.0 * math.pi / lon_count)
    norm_scale = 1.0 / math.sqrt(lon_count)
    return jnp.stack([jnp.cos(radians) * norm_scale, -jnp.sin(radians) * norm_scale], 1).astype(jnp.bfloat16)

def damping(waves, damp_rates, columns):
    half_cols = columns // 2
    col_index = jnp.arange(columns, dtype=jnp.int32)
    offset = jnp.where(col_index < half_cols, 2 * col_index, 2 * col_index - columns + 1)
    degree = waves[:, None] + offset[None, :]
    degree_ratio = (degree * (degree + 1)).astype(jnp.float32) / float(LMAX * (LMAX + 1))
    factor = 1.0 / (1.0 + damp_rates[None, :, None] * (degree_ratio ** 4)[:, None, :])
    return jnp.where((degree <= LMAX)[:, None, :], factor, 0.0)

def reference(grid_in, legendre, wave_slot, lat_modes, gauss_weight, diffusion):
    highest = lax.Precision.HIGHEST
    angles = angle_table(wave_slot, NLON)
    keep_mask = (wave_slot[:, None] < lat_modes[None, :]).astype(jnp.float32)
    fourier = jnp.einsum('fjx,xrs->rsfj', grid_in.astype(jnp.float32), angles.astype(jnp.float32), precision=highest)
    fourier = (fourier * keep_mask[None, :, None, :]).astype(jnp.bfloat16)
    half_cols = MW // 2
    half_lats = NLAT // 2

    def per_slot(slot_items):
        slot_data, tables, slot_wave = slot_items
        north_half = slot_data[..., :half_lats].astype(jnp.float32)
        south_half = jnp.flip(slot_data[..., half_lats:], -1).astype(jnp.float32)
        even_part = ((north_half + south_half) * gauss_weight).astype(jnp.bfloat16)
        odd_part = ((north_half - south_half) * gauss_weight).astype(jnp.bfloat16)
        table_wide = tables.astype(jnp.float32)
        even_cols = jnp.einsum('rfj,jq->rfq', even_part.astype(jnp.float32), table_wide[:, :half_cols], precision=highest)
        odd_cols = jnp.einsum('rfj,jq->rfq', odd_part.astype(jnp.float32), table_wide[:, half_cols:], precision=highest)
        raw_coeff = jnp.concatenate([even_cols, odd_cols], -1)
        spectra = raw_coeff * damping(slot_wave[None], diffusion, MW)[0][None]
        rounded = spectra.astype(jnp.bfloat16).astype(jnp.float32)
        sym_part = jnp.einsum('rfq,jq->rfj', rounded[..., :half_cols], table_wide[:, :half_cols], precision=highest)
        anti_part = jnp.einsum('rfq,jq->rfj', rounded[..., half_cols:], table_wide[:, half_cols:], precision=highest)
        synthesized = jnp.concatenate([(sym_part + anti_part).astype(jnp.bfloat16), jnp.flip((sym_part - anti_part).astype(jnp.bfloat16), -1)], -1)
        return (spectra, synthesized)
    spectra, synthesized = lax.map(per_slot, (jnp.moveaxis(fourier, 1, 0), legendre, wave_slot))
    spectra = jnp.moveaxis(spectra, 0, 1)
    masked = synthesized.astype(jnp.float32) * keep_mask[:, None, None, :]
    grid_out = 2.0 * jnp.einsum('srfj,xrs->fjx', masked, angles.astype(jnp.float32), precision=highest)
    return (grid_out, spectra)
```

```python
import functools
import math

import jax
import jax.numpy as jnp
from jax import lax
from jax.experimental import pallas as pl
from jax.experimental.pallas import tpu as pltpu
from jax.sharding import PartitionSpec as P

LMAX = 1279
LANES = 128
HALF = 64
GROUP = 8
BF = jnp.bfloat16
F32 = jnp.float32
VMEM_BYTES = 60 * 1024 * 1024


def dot(a, b):
    return jnp.dot(a, b, preferred_element_type=F32)


def dot_t(a, b):
    return lax.dot_general(a, b, (((1,), (1,)), ((), ())), preferred_element_type=F32)


def angle_kernel(cos_a, sin_a, cos_b, sin_b, out):
    cb, sb = cos_b[...], sin_b[...]
    for a in range(out.shape[1] // LANES):
        ca = cos_a[:, a : a + 1]
        sa = sin_a[:, a : a + 1]
        out[:, a * LANES : (a + 1) * LANES] = (ca * cb - sa * sb).astype(BF)


def angle_rows(waves, lon_count):
    rows = 2 * waves.shape[0]
    tiles = lon_count // LANES
    wave_row = jnp.repeat(waves, 2)[:, None]
    quarter = (jnp.arange(rows, dtype=jnp.int32) % 2)[:, None] * (lon_count // 4)
    coarse = jnp.arange(LANES, dtype=jnp.int32)[None, :] * LANES
    fine = jnp.arange(LANES, dtype=jnp.int32)[None, :]
    unit = 2.0 * math.pi / lon_count
    phase_a = ((wave_row * coarse + quarter) % lon_count).astype(F32) * unit
    phase_b = (wave_row * fine % lon_count).astype(F32) * unit
    scale = 1.0 / math.sqrt(lon_count)
    step = 256
    spec = pl.BlockSpec((step, LANES), lambda i: (i, 0))
    return pl.pallas_call(
        angle_kernel,
        grid=(rows // step,),
        in_specs=[spec] * 4,
        out_specs=pl.BlockSpec((step, tiles * LANES), lambda i: (i, 0)),
        out_shape=jax.ShapeDtypeStruct((rows, lon_count), BF),
        cost_estimate=pl.CostEstimate(
            flops=4 * rows * lon_count, bytes_accessed=2 * rows * lon_count, transcendentals=0
        ),
        name="angles",
    )(jnp.cos(phase_a), jnp.sin(phase_a), jnp.cos(phase_b) * scale, jnp.sin(phase_b) * scale)


def dft_kernel(starts, field_a, field_b, angles, wave_row, modes, out, arranged):
    first, second, rest = (pl.multiple_of(starts[i], HALF) for i in range(3))
    for i, field in enumerate((field_a, field_b)):
        arranged[i * 256 : i * 256 + 128] = field[0, pl.ds(first, 128), :]
        arranged[i * 256 + 128 : i * 256 + 256] = field[0, pl.ds(second, 128), :]
        arranged[512 + i * HALF : 512 + (i + 1) * HALF] = field[0, pl.ds(rest, HALF), :]
    dests, rows, width = out.shape
    per = 8
    count = per * rows

    @pl.loop(0, dests // per)
    def _(i):
        at = pl.ds(pl.multiple_of(i * count, 16), count)
        value = dot_t(angles[at, :], arranged[...])
        value = jnp.where(wave_row[at, :] < modes[...], value, 0.0)
        out[pl.ds(i * per, per)] = value.astype(BF).reshape(per, rows, width)


def dft(grid_in, angles, wave_row, modes, starts, dests):
    fields, lats, lon = grid_in.shape
    pairs = fields // 2
    rows = angles.shape[0]
    width = 2 * lats
    flops = 2 * rows * fields * lats * lon
    return pl.pallas_call(
        dft_kernel,
        grid_spec=pltpu.PrefetchScalarGridSpec(
            num_scalar_prefetch=1,
            grid=(pairs,),
            in_specs=[
                pl.BlockSpec((1, lats, lon), lambda k, s: (k, 0, 0)),
                pl.BlockSpec((1, lats, lon), lambda k, s: (k + pairs, 0, 0)),
                pl.BlockSpec((rows, lon), lambda k, s: (0, 0)),
                pl.BlockSpec((rows, 1), lambda k, s: (0, 0)),
                pl.BlockSpec((1, width), lambda k, s: (0, 0)),
            ],
            out_specs=pl.BlockSpec((dests, rows // dests, width), lambda k, s: (0, 0, k)),
            scratch_shapes=[pltpu.VMEM((width, lon), BF)],
        ),
        out_shape=jax.ShapeDtypeStruct((dests, rows // dests, pairs * width), BF),
        compiler_params=pltpu.CompilerParams(vmem_limit_bytes=VMEM_BYTES),
        cost_estimate=pl.CostEstimate(
            flops=flops, bytes_accessed=2 * fields * lats * (lon + rows), transcendentals=0
        ),
        name="dft",
    )(starts, grid_in, grid_in, angles, wave_row, modes)


def inverse_kernel(starts, back, angles, wave_row, modes, out_a, out_b, turned):
    first, second, rest = (pl.multiple_of(starts[i], HALF) for i in range(3))
    dests, rows, width = back.shape
    per = 8
    count = per * rows
    for i in range(dests // per):
        value = back[i * per : (i + 1) * per].reshape(count, width).astype(F32)
        value = jnp.where(wave_row[i * count : (i + 1) * count, :] < modes[...], value, 0.0)
        turned[:, i * count : (i + 1) * count] = value.T.astype(BF)
    lon = angles.shape[1]
    step = 3 * LANES

    @pl.loop(0, lon // step)
    def _(n):
        cols = pl.ds(pl.multiple_of(n * step, LANES), step)
        value = 2.0 * dot(turned[...], angles[:, cols])
        for i, out in enumerate((out_a, out_b)):
            out[0, pl.ds(first, 128), cols] = value[i * 256 : i * 256 + 128]
            out[0, pl.ds(second, 128), cols] = value[i * 256 + 128 : i * 256 + 256]
            out[0, pl.ds(rest, HALF), cols] = value[512 + i * HALF : 512 + (i + 1) * HALF]


def inverse_kernel_joined(starts, back, angles, wave_row, modes, out, turned):
    inverse_kernel(starts, back, angles, wave_row, modes, out.at[0], out.at[1], turned)


def inverse_dft(back, angles, wave_row, modes, starts, fields, lats):
    dests, rows, _ = back.shape
    pairs = fields // 2
    lon = angles.shape[1]
    width = 2 * lats
    flops = 2 * dests * rows * fields * lats * lon
    out = pl.pallas_call(
        inverse_kernel_joined,
        grid_spec=pltpu.PrefetchScalarGridSpec(
            num_scalar_prefetch=1,
            grid=(pairs,),
            in_specs=[
                pl.BlockSpec((dests, rows, width), lambda k, s: (0, 0, k)),
                pl.BlockSpec((dests * rows, lon), lambda k, s: (0, 0)),
                pl.BlockSpec((dests * rows, 1), lambda k, s: (0, 0)),
                pl.BlockSpec((1, width), lambda k, s: (0, 0)),
            ],
            out_specs=pl.BlockSpec((2, 1, lats, lon), lambda k, s: (0, k, 0, 0)),
            scratch_shapes=[pltpu.VMEM((width, dests * rows), BF)],
        ),
        out_shape=jax.ShapeDtypeStruct((2, pairs, lats, lon), F32),
        compiler_params=pltpu.CompilerParams(vmem_limit_bytes=VMEM_BYTES),
        cost_estimate=pl.CostEstimate(
            flops=flops, bytes_accessed=fields * lats * (4 * lon + 2 * dests * rows), transcendentals=0
        ),
        name="inverse_dft",
    )(starts, back, angles, wave_row, modes)
    return out.reshape(fields, lats, lon)


def legendre_kernel(
    lat_count,
    fld_count,
    lats,
    half_cols,
    arrived,
    low,
    h0,
    h1,
    h2,
    h3,
    degree4,
    rates,
    weights,
    gather,
    scatter,
    mirror,
    spectra,
    leaving,
    even,
    odd,
    north,
    south,
):
    pair = pl.program_id(1)
    blocks = lat_count // 2
    width = 2 * lats
    pairs = arrived.shape[2] // width
    slot_rows = 2 * fld_count * pairs
    lower = lax.broadcasted_iota(jnp.int32, (GROUP * slot_rows, LANES), 1) < HALF
    flip_tile = mirror[0]
    flip_half = mirror[1]

    def swap(x):
        return pltpu.roll(x, HALF, 1)

    def put(ref, half, at, x):
        ref[:, half * slot_rows : (half + 1) * slot_rows, at : at + LANES] = x.astype(BF).reshape(
            GROUP, slot_rows, LANES
        )

    def get(ref, half, at):
        return ref[:, half * slot_rows : (half + 1) * slot_rows, at : at + LANES].reshape(
            GROUP * slot_rows, LANES
        )

    def stacked(lat):
        parts = [
            arrived[lat * fld_count + f, :, k * width : (k + 1) * width]
            for f in range(fld_count)
            for k in range(pairs)
        ]
        return dot(gather[...], jnp.concatenate(parts, 0))

    @pl.when(pair == 0)
    def _():
        rests = []
        for block in range(blocks):
            up = stacked(block)
            down = stacked(lat_count - 1 - block).astype(BF)
            for piece in range(5):
                tile = slice(piece * LANES, (piece + 1) * LANES)
                n = up[:, tile]
                s = dot(down[:, tile], flip_tile if piece < 4 else flip_half)
                w = weights[block : block + 1, 2 * LANES :] if piece == 4 else (
                    weights[block : block + 1, (piece % 2) * LANES : (piece % 2 + 1) * LANES]
                )
                e, o = (n + s) * w, (n - s) * w
                if piece < 4:
                    at = block * 256 + (piece % 2) * LANES
                    put(even, piece // 2, at, e)
                    put(odd, piece // 2, at, o)
                else:
                    rests.append((e, o))
        for b in range(blocks // 2):
            at = blocks * 256 + b * LANES
            for ref, c in ((even, 0), (odd, 1)):
                x, y = rests[2 * b][c], rests[2 * b + 1][c]
                put(ref, 0, at, jnp.where(lower, x, swap(y)))
                put(ref, 1, at, jnp.where(lower, swap(x), y))

    def rows_of(load):
        parts = [load(b * lats, 256) for b in range(blocks)]
        parts.append(jnp.concatenate([load(b * lats + 256, HALF) for b in range(blocks)], 0))
        return parts

    def transform(slot, local, even_table, odd_table, cols):
        def project(ref, parts):
            total = None
            for i, part in enumerate(parts):
                term = dot(ref[slot, :, i * 256 : i * 256 + part.shape[0]], part)
                total = term if total is None else total + term
            return total

        results = []
        tables = []
        for c, (ref, load) in enumerate(((even, even_table), (odd, odd_table))):
            parts = rows_of(load)
            tables.append(parts)
            d4 = degree4[local, :, c * half_cols : c * half_cols + cols]
            factor = jnp.where(d4 >= 0.0, 1.0 / (1.0 + rates[...] * d4), 0.0)
            results.append(project(ref, parts) * factor)
        for c, value in enumerate(results):
            for f in range(fld_count):
                for r in range(2):
                    at = (f * 2 + r) * pairs
                    both = jnp.concatenate(
                        [value[at : at + pairs], value[slot_rows + at : slot_rows + at + pairs]], 0
                    )
                    spectra[f, r, local, :, c * half_cols : c * half_cols + cols] = both
                    if cols < half_cols:
                        spectra[f, r, local, :, c * half_cols + cols : (c + 1) * half_cols] = (
                            jnp.zeros((2 * pairs, half_cols - cols), F32)
                        )
        coeff = [v.astype(BF) for v in results]
        for i in range(blocks + 1):
            sym = dot_t(coeff[0], tables[0][i])
            anti = dot_t(coeff[1], tables[1][i])
            at = slice(i * 256, i * 256 + sym.shape[1])
            north[slot, :, at] = (sym + anti).astype(BF)
            south[slot, :, at] = (sym - anti).astype(BF)

    transform(
        2 * pair,
        0,
        lambda at, n: low[0, at : at + n, :half_cols],
        lambda at, n: low[0, at : at + n, half_cols:],
        half_cols,
    )
    transform(
        2 * pair + 1,
        1,
        lambda at, n: jnp.concatenate([h0[0, at : at + n, :], h1[0, at : at + n, :]], 1),
        lambda at, n: jnp.concatenate([h2[0, at : at + n, :], h3[0, at : at + n, :]], 1),
        2 * LANES,
    )

    @pl.when(pair == pl.num_programs(1) - 1)
    def _():
        for block in range(blocks):
            for ref, lat in ((north, block), (south, lat_count - 1 - block)):
                pieces = [
                    get(ref, half, block * 256 + t * LANES) for half in range(2) for t in range(2)
                ]
                at = blocks * 256 + (block // 2) * LANES
                x, y = get(ref, 0, at).astype(F32), get(ref, 1, at).astype(F32)
                rest = jnp.where(lower, x, swap(y)) if block % 2 == 0 else jnp.where(lower, swap(x), y)
                pieces.append(rest.astype(BF))
                if ref is south:
                    pieces = [
                        dot(p, flip_tile if i < 4 else flip_half).astype(BF)
                        for i, p in enumerate(pieces)
                    ]
                joined = dot(scatter[...], jnp.concatenate(pieces, 1)).astype(BF)
                for f in range(fld_count):
                    for k in range(pairs):
                        row = (f * pairs + k) * 2 * GROUP
                        leaving[lat * fld_count + f, :, k * width : (k + 1) * width] = joined[
                            row : row + 2 * GROUP
                        ]


def legendre_step(arrived, tables, own_waves, damp_rates, gauss_weight, lat_count, fld_count):
    slots, half_lats, columns = tables.shape
    half_cols = columns // 2
    sources, _, wide = arrived.shape
    lats = 2 * half_lats // lat_count
    width = 2 * lats
    pairs = wide // width
    slot_rows = 2 * fld_count * pairs
    rows = 2 * slot_rows
    blocks = lat_count // 2
    groups, inner = slots // GROUP, GROUP // 2

    col_index = jnp.arange(columns, dtype=jnp.int32)
    offset = jnp.where(col_index < half_cols, 2 * col_index, 2 * col_index - columns + 1)
    degree = own_waves[:, None] + offset[None, :]
    ratio = (degree * (degree + 1)).astype(F32) / float(LMAX * (LMAX + 1))
    degree4 = jnp.where(degree <= LMAX, ratio**4, -1.0)[:, None, :]

    by_field = damp_rates.reshape(fld_count, 2, pairs)
    rates = jnp.broadcast_to(
        by_field.transpose(1, 0, 2)[:, :, None, :], (2, fld_count, 2, pairs)
    ).reshape(rows, 1)
    w = gauss_weight.reshape(blocks, lats)
    weights = jnp.concatenate([w, w[:, 256:]], 1)

    size = GROUP * slot_rows
    target = jnp.arange(size, dtype=jnp.int32)
    s, rest = target // slot_rows, target % slot_rows
    f, rest = rest // (2 * pairs), rest % (2 * pairs)
    r, k = rest // pairs, rest % pairs
    source = ((f * pairs + k) * GROUP + s) * 2 + r
    gather = (source[:, None] == target[None, :]).astype(BF)
    scatter = (source[None, :] == target[:, None]).astype(BF)
    lane = jnp.arange(LANES, dtype=jnp.int32)
    place = lane[:, None] + lane[None, :]
    same_half = lane[:, None] // HALF == lane[None, :] // HALF
    mirror = jnp.stack(
        [place == LANES - 1, same_half & (place % LANES == HALF - 1)]
    ).astype(BF)

    def slot_of(g, p):
        return g * GROUP + 2 * p

    narrow = [
        pl.BlockSpec((1, half_lats, LANES), functools.partial(lambda t, g, p: (slot_of(g, p) + 1, 0, t), t))
        for t in (0, 1, half_cols // LANES, half_cols // LANES + 1)
    ]
    whole = lambda *shape: pl.BlockSpec(shape, lambda g, p: (0,) * len(shape))
    scratch = pltpu.VMEM((GROUP, rows, half_lats), BF)
    flops = 2 * 2 * slots * rows * half_lats * columns
    return pl.pallas_call(
        functools.partial(legendre_kernel, lat_count, fld_count, lats, half_cols),
        grid=(groups, inner),
        in_specs=[
            pl.BlockSpec((sources, 2 * GROUP, wide), lambda g, p: (0, g, 0)),
            pl.BlockSpec((1, half_lats, columns), lambda g, p: (slot_of(g, p), 0, 0)),
            *narrow,
            pl.BlockSpec((2, 1, columns), lambda g, p: (g * inner + p, 0, 0)),
            whole(rows, 1),
            whole(blocks, 3 * LANES),
            whole(size, size),
            whole(size, size),
            whole(2, LANES, LANES),
        ],
        out_specs=[
            pl.BlockSpec(
                (fld_count, 2, 2, 2 * pairs, columns), lambda g, p: (0, 0, g * inner + p, 0, 0)
            ),
            pl.BlockSpec((sources, 2 * GROUP, wide), lambda g, p: (0, g, 0)),
        ],
        out_shape=[
            jax.ShapeDtypeStruct((fld_count, 2, slots, 2 * pairs, columns), F32),
            jax.ShapeDtypeStruct(arrived.shape, BF),
        ],
        scratch_shapes=[scratch] * 4,
        compiler_params=pltpu.CompilerParams(vmem_limit_bytes=VMEM_BYTES),
        cost_estimate=pl.CostEstimate(
            flops=flops, bytes_accessed=2 * slots * half_lats * columns, transcendentals=0
        ),
        name="legendre",
    )(arrived, tables, *[tables] * 4, degree4, rates, weights, gather, scatter, mirror)


def fast_body(grid_in, legendre, wave_slot, lat_modes, gauss_weight, diffusion):
    fields, lats, lon = grid_in.shape
    slots_all = wave_slot.shape[0]
    lat_count = lax.axis_size("lat")
    fld_count = lax.axis_size("fld")
    owners = lat_count * fld_count
    owned = slots_all // owners
    lat_index = lax.axis_index("lat")
    owner = lat_index * fld_count + lax.axis_index("fld")
    southern = lat_index >= lat_count // 2
    starts = jnp.where(southern, jnp.array([192, 64, 0]), jnp.array([0, 128, 256])).astype(jnp.int32)
    flipped = jnp.concatenate([lat_modes[192:], lat_modes[64:192], lat_modes[:64]])
    ordered = jnp.where(southern, flipped, lat_modes)
    modes = jnp.concatenate([ordered[:256], ordered[:256], ordered[256:], ordered[256:]])[None, :]
    wave_row = jnp.repeat(wave_slot, 2)[:, None]
    own_waves = lax.dynamic_slice_in_dim(wave_slot, owner * owned, owned)

    angles = angle_rows(wave_slot, lon)
    sent = dft(grid_in, angles, wave_row, modes, starts, owners)
    arrived = lax.all_to_all(sent, ("lat", "fld"), 0, 0, tiled=True)
    spectra, leaving = legendre_step(
        arrived, legendre, own_waves, diffusion, gauss_weight, lat_count, fld_count
    )
    back = lax.all_to_all(leaving, ("lat", "fld"), 0, 0, tiled=True)
    spectra = lax.all_to_all(spectra, "fld", 0, 0, tiled=True)
    spectra = spectra.transpose(1, 0, 2, 3, 4).reshape(2, fld_count * owned, fields, -1)
    grid_out = inverse_dft(back, angles, wave_row, modes, starts, fields, lats)
    return (grid_out, spectra)


def angle_table(waves, lon_count):
    points = jnp.arange(lon_count, dtype=jnp.int32)
    phase_index = points[:, None] * waves[None, :] % lon_count
    radians = phase_index.astype(jnp.float32) * (2.0 * math.pi / lon_count)
    norm_scale = 1.0 / math.sqrt(lon_count)
    return jnp.stack([jnp.cos(radians) * norm_scale, -jnp.sin(radians) * norm_scale], 1).astype(
        jnp.bfloat16
    )


def damping(waves, damp_rates, columns):
    half_cols = columns // 2
    col_index = jnp.arange(columns, dtype=jnp.int32)
    offset = jnp.where(col_index < half_cols, 2 * col_index, 2 * col_index - columns + 1)
    degree = waves[:, None] + offset[None, :]
    degree_ratio = (degree * (degree + 1)).astype(jnp.float32) / float(LMAX * (LMAX + 1))
    factor = 1.0 / (1.0 + damp_rates[None, :, None] * (degree_ratio**4)[:, None, :])
    return jnp.where((degree <= LMAX)[:, None, :], factor, 0.0)


def project(even_part, odd_part, tables, used_cols):
    half_cols = tables.shape[2] // 2
    even_cols = jnp.einsum(
        "rsfj,sjq->rsfq", even_part, tables[:, :, :used_cols], preferred_element_type=jnp.float32
    )
    odd_cols = jnp.einsum(
        "rsfj,sjq->rsfq",
        odd_part,
        tables[:, :, half_cols : half_cols + used_cols],
        preferred_element_type=jnp.float32,
    )
    return jnp.concatenate([even_cols, odd_cols], -1)


def expand(rounded, tables, used_cols):
    half_cols = tables.shape[2] // 2
    sym_part = jnp.einsum(
        "rsfq,sjq->rsfj",
        rounded[..., :used_cols],
        tables[:, :, :used_cols],
        preferred_element_type=jnp.float32,
    )
    anti_part = jnp.einsum(
        "rsfq,sjq->rsfj",
        rounded[..., half_cols : half_cols + used_cols],
        tables[:, :, half_cols : half_cols + used_cols],
        preferred_element_type=jnp.float32,
    )
    return (sym_part, anti_part)


def transform_block(block_data, tables, block_waves, damp_rates, weights):
    half_lats = weights.shape[0]
    columns = tables.shape[2]
    half_cols = columns // 2
    north_half = block_data[..., :half_lats].astype(jnp.float32)
    south_half = jnp.flip(block_data[..., half_lats:], -1).astype(jnp.float32)
    even_part = ((north_half + south_half) * weights).astype(jnp.bfloat16)
    odd_part = ((north_half - south_half) * weights).astype(jnp.bfloat16)
    raw_coeff = project(even_part, odd_part, tables, half_cols)
    spectra = raw_coeff * damping(block_waves, damp_rates, columns)[None]
    rounded = spectra.astype(jnp.bfloat16)
    sym_part, anti_part = expand(rounded, tables, half_cols)
    synthesized = jnp.concatenate(
        [
            (sym_part + anti_part).astype(jnp.bfloat16),
            jnp.flip((sym_part - anti_part).astype(jnp.bfloat16), -1),
        ],
        -1,
    )
    return (spectra, synthesized)


def general_body(grid_in, legendre, wave_slot, lat_modes, gauss_weight, diffusion):
    fld_dev, lat_dev, lon_count = grid_in.shape
    slots_all = wave_slot.shape[0]
    lat_count = lax.axis_size("lat")
    fld_count = lax.axis_size("fld")
    lat_total = lat_dev * lat_count
    lat_index = lax.axis_index("lat")
    fld_index = lax.axis_index("fld")
    owned_slots = slots_all // (lat_count * fld_count)
    angles = angle_table(wave_slot, lon_count)
    keep_mask = (wave_slot[:, None] < lat_modes[None, :]).astype(jnp.float32)
    fourier = jnp.einsum("fjx,xrs->rsfj", grid_in, angles, preferred_element_type=jnp.float32)
    fourier = (fourier * keep_mask[None, :, None, :]).astype(jnp.bfloat16)
    own_waves = lax.dynamic_slice_in_dim(
        wave_slot, (lat_index * fld_count + fld_index) * owned_slots, owned_slots
    )
    flattened = fourier.reshape(2, slots_all, fld_dev * lat_dev)
    arrived = lax.all_to_all(flattened, ("lat", "fld"), split_axis=1, concat_axis=2, tiled=True)
    arrived = arrived.reshape(2, owned_slots, lat_count, fld_count, fld_dev, lat_dev)
    arrived = arrived.transpose(0, 1, 3, 4, 2, 5).reshape(
        2, owned_slots, fld_count * fld_dev, lat_total
    )
    owned_spectra, synthesized = transform_block(
        arrived, legendre, own_waves, diffusion, gauss_weight
    )
    spectra = lax.all_to_all(owned_spectra, "fld", split_axis=2, concat_axis=1, tiled=True)
    outgoing = synthesized.reshape(2, owned_slots, fld_count, fld_dev, lat_count, lat_dev)
    outgoing = outgoing.transpose(0, 1, 4, 2, 3, 5).reshape(
        2, owned_slots, lat_count * fld_count * fld_dev * lat_dev
    )
    returned = lax.all_to_all(outgoing, ("lat", "fld"), split_axis=2, concat_axis=1, tiled=True)
    returned = returned.reshape(2, slots_all, fld_dev, lat_dev)
    keep_narrow = keep_mask.astype(jnp.bfloat16)
    masked = returned * keep_narrow[None, :, None, :]
    grid_out = 2.0 * jnp.einsum("rsfj,xrs->fjx", masked, angles, preferred_element_type=jnp.float32)
    return (grid_out, spectra)


def body(grid_in, legendre, wave_slot, lat_modes, gauss_weight, diffusion):
    fields, lats, lon = grid_in.shape
    slots, _, columns = legendre.shape
    lat_count = lax.axis_size("lat")
    fits = (
        lats == 2 * LANES + HALF
        and lat_count % 4 == 0
        and fields == 8
        and slots % GROUP == 0
        and lon % (3 * LANES) == 0
        and columns == 6 * LANES
    )
    chosen = fast_body if fits else general_body
    return chosen(grid_in, legendre, wave_slot, lat_modes, gauss_weight, diffusion)


def solution(mesh):
    return jax.shard_map(
        body,
        mesh=mesh,
        in_specs=(P("fld", "lat", None), P(("lat", "fld"), None, None), P(), P("lat"), P(), P()),
        out_specs=(P("fld", "lat", None), P(None, "lat", "fld", None)),
        check_vma=False,
    )
```

```python
import functools
import math

import jax
import jax.numpy as jnp
from jax import lax
from jax.experimental import pallas as pl
from jax.experimental.pallas import tpu as pltpu
from jax.sharding import PartitionSpec as P

LMAX = 1279
LANES = 128
HALF = 64
GROUP = 8
CHUNKS = 2
BF = jnp.bfloat16
F32 = jnp.float32
VMEM_BYTES = 60 * 1024 * 1024


def dot(a, b):
    return jnp.dot(a, b, preferred_element_type=F32)


def dot_t(a, b):
    return lax.dot_general(a, b, (((1,), (1,)), ((), ())), preferred_element_type=F32)


def turn_cos(phase, count):
    whole = phase - jnp.floor(phase * (1.0 / count) + 0.5) * count
    x = whole * (2.0 * math.pi / count)
    square = x * x
    total = jnp.full_like(square, 1.0 / math.factorial(18) * -1.0)
    for order in range(16, -1, -2):
        total = total * square + (-1.0) ** (order // 2) / math.factorial(order)
    return total


def angle_kernel(lon, wave_row, out):
    rows = out.shape[0]
    step = 64
    scale = 1.0 / math.sqrt(lon)
    quarter = lon // 4

    @pl.loop(0, rows // step)
    def _(i):
        at = pl.ds(pl.multiple_of(i * step, step), step)
        wave = wave_row[at, :].astype(F32)
        lane = lax.broadcasted_iota(jnp.int32, (step, LANES), 1).astype(F32)
        part = lax.broadcasted_iota(jnp.int32, (step, LANES), 0)
        turn = (part % 2 * quarter).astype(F32)
        fine = wave * lane
        coarse = fine * LANES + turn
        cos_b = turn_cos(fine, lon) * scale
        sin_b = turn_cos(fine - quarter, lon) * scale
        cos_a = turn_cos(coarse, lon)
        sin_a = turn_cos(coarse - quarter, lon)
        for a in range(lon // LANES):
            value = cos_a[:, a : a + 1] * cos_b - sin_a[:, a : a + 1] * sin_b
            out[at, a * LANES : (a + 1) * LANES] = value.astype(BF)


def angle_rows(wave_row, lon):
    rows = wave_row.shape[0]
    step = 256
    return pl.pallas_call(
        functools.partial(angle_kernel, lon),
        grid=(rows // step,),
        in_specs=[pl.BlockSpec((step, 1), lambda i: (i, 0))],
        out_specs=pl.BlockSpec((step, lon), lambda i: (i, 0)),
        out_shape=jax.ShapeDtypeStruct((rows, lon), BF),
        cost_estimate=pl.CostEstimate(
            flops=4 * rows * lon, bytes_accessed=2 * rows * lon, transcendentals=0
        ),
        name="angles",
    )(wave_row)


def dft_kernel(count, starts, *refs):
    fields = refs[:count]
    angles, wave_row, modes, out, arranged = refs[count:]
    pairs = count // 2
    width = out.shape[2] // pairs

    @pl.when(pl.program_id(0) == 0)
    def _():
        first, second, rest = (pl.multiple_of(starts[i], HALF) for i in range(3))
        for i, field in enumerate(fields):
            half, pair = divmod(i, pairs)
            at = pair * width + half * 256
            arranged[at : at + 128] = field[0, pl.ds(first, 128), :]
            arranged[at + 128 : at + 256] = field[0, pl.ds(second, 128), :]
            at = pair * width + 512 + half * HALF
            arranged[at : at + HALF] = field[0, pl.ds(rest, HALF), :]

    value = dot_t(angles[...], arranged[...])
    value = jnp.where(wave_row[...] < modes[...], value, 0.0)
    out[...] = value.astype(BF).reshape(out.shape)


def dft(grid_in, angles, wave_row, modes, starts, dests, chunk, chunks):
    fields, lats, lon = grid_in.shape
    count = fields // chunks
    rows = angles.shape[0]
    wide = count * lats
    per = dests // 2
    tile = rows * per // dests
    return pl.pallas_call(
        functools.partial(dft_kernel, count),
        grid_spec=pltpu.PrefetchScalarGridSpec(
            num_scalar_prefetch=1,
            grid=(dests // per,),
            in_specs=[
                *[
                    pl.BlockSpec(
                        (1, lats, lon), functools.partial(lambda f, i, s: (f, 0, 0), chunk * count + f)
                    )
                    for f in range(count)
                ],
                pl.BlockSpec((tile, lon), lambda i, s: (i, 0)),
                pl.BlockSpec((tile, 1), lambda i, s: (i, 0)),
                pl.BlockSpec((1, wide), lambda i, s: (0, 0)),
            ],
            out_specs=pl.BlockSpec((per, rows // dests, wide), lambda i, s: (i, 0, 0)),
            scratch_shapes=[pltpu.VMEM((wide, lon), BF)],
        ),
        out_shape=jax.ShapeDtypeStruct((dests, rows // dests, wide), BF),
        compiler_params=pltpu.CompilerParams(vmem_limit_bytes=VMEM_BYTES),
        cost_estimate=pl.CostEstimate(
            flops=2 * rows * wide * lon, bytes_accessed=2 * wide * (lon + rows), transcendentals=0
        ),
        name="dft",
    )(starts, *[grid_in] * count, angles, wave_row, modes)


def inverse_kernel(starts, back, angles, wave_row, modes, *refs):
    out, turned = refs[-2:]
    first, second, rest = (pl.multiple_of(starts[i], HALF) for i in range(3))
    dests, rows, width = back.shape
    per = 8
    count = per * rows
    for i in range(dests // per):
        value = back[i * per : (i + 1) * per].reshape(count, width).astype(F32)
        value = jnp.where(wave_row[i * count : (i + 1) * count, :] < modes[...], value, 0.0)
        turned[:, i * count : (i + 1) * count] = value.T.astype(BF)
    lon = angles.shape[1]
    step = 6 * LANES
    for at in range(0, lon, step):
        cols = slice(at, min(at + step, lon))
        value = 2.0 * dot(turned[...], angles[:, cols])
        for i in range(2):
            out[0, i, 0, pl.ds(first, 128), cols] = value[i * 256 : i * 256 + 128]
            out[0, i, 0, pl.ds(second, 128), cols] = value[i * 256 + 128 : i * 256 + 256]
            out[0, i, 0, pl.ds(rest, HALF), cols] = value[512 + i * HALF : 512 + (i + 1) * HALF]


def inverse_dft(back, angles, wave_row, modes, starts, lats, whole, chunk, chunks):
    dests, rows, wide = back.shape
    lon = angles.shape[1]
    width = 2 * lats
    pairs = wide // width
    given = [] if whole is None else [whole]
    return pl.pallas_call(
        inverse_kernel,
        grid_spec=pltpu.PrefetchScalarGridSpec(
            num_scalar_prefetch=1,
            grid=(pairs,),
            in_specs=[
                pl.BlockSpec((dests, rows, width), lambda k, s: (0, 0, k)),
                pl.BlockSpec((dests * rows, lon), lambda k, s: (0, 0)),
                pl.BlockSpec((dests * rows, 1), lambda k, s: (0, 0)),
                pl.BlockSpec((1, width), lambda k, s: (0, 0)),
                *[pl.BlockSpec(memory_space=pl.ANY) for _ in given],
            ],
            out_specs=pl.BlockSpec((1, 2, 1, lats, lon), lambda k, s: (chunk, 0, k, 0, 0)),
            scratch_shapes=[pltpu.VMEM((width, dests * rows), BF)],
        ),
        out_shape=jax.ShapeDtypeStruct((chunks, 2, pairs, lats, lon), F32),
        input_output_aliases={5: 0} if given else {},
        compiler_params=pltpu.CompilerParams(vmem_limit_bytes=VMEM_BYTES),
        cost_estimate=pl.CostEstimate(
            flops=2 * dests * rows * wide * lon,
            bytes_accessed=wide * (4 * lon + 2 * dests * rows),
            transcendentals=0,
        ),
        name="inverse_dft",
    )(starts, back, angles, wave_row, modes[:, :width], *given)


def legendre_kernel(
    lat_count,
    fld_count,
    lats,
    half_cols,
    arrived,
    low,
    h0,
    h1,
    h2,
    h3,
    degree4,
    rates,
    weights,
    gather,
    scatter,
    mirror,
    spectra,
    leaving,
    even,
    odd,
    north,
    south,
):
    pair = pl.program_id(1)
    blocks = lat_count // 2
    width = 2 * lats
    pairs = arrived.shape[2] // width
    slot_rows = 2 * fld_count * pairs
    lower = lax.broadcasted_iota(jnp.int32, (GROUP * slot_rows, LANES), 1) < HALF
    flip_tile = mirror[0]
    flip_half = mirror[1]

    def swap(x):
        return pltpu.roll(x, HALF, 1)

    def put(ref, half, at, x):
        ref[:, half * slot_rows : (half + 1) * slot_rows, at : at + LANES] = x.astype(BF).reshape(
            GROUP, slot_rows, LANES
        )

    def get(ref, half, at):
        return ref[:, half * slot_rows : (half + 1) * slot_rows, at : at + LANES].reshape(
            GROUP * slot_rows, LANES
        )

    def stacked(lat):
        parts = [
            arrived[lat * fld_count + f, :, k * width : (k + 1) * width]
            for f in range(fld_count)
            for k in range(pairs)
        ]
        return dot(gather[...], jnp.concatenate(parts, 0))

    @pl.when(pair == 0)
    def _():
        rests = []
        for block in range(blocks):
            up = stacked(block)
            down = stacked(lat_count - 1 - block).astype(BF)
            for piece in range(5):
                tile = slice(piece * LANES, (piece + 1) * LANES)
                n = up[:, tile]
                s = dot(down[:, tile], flip_tile if piece < 4 else flip_half)
                w = weights[block : block + 1, 2 * LANES :] if piece == 4 else (
                    weights[block : block + 1, (piece % 2) * LANES : (piece % 2 + 1) * LANES]
                )
                e, o = (n + s) * w, (n - s) * w
                if piece < 4:
                    at = block * 256 + (piece % 2) * LANES
                    put(even, piece // 2, at, e)
                    put(odd, piece // 2, at, o)
                else:
                    rests.append((e, o))
        for b in range(blocks // 2):
            at = blocks * 256 + b * LANES
            for ref, c in ((even, 0), (odd, 1)):
                x, y = rests[2 * b][c], rests[2 * b + 1][c]
                put(ref, 0, at, jnp.where(lower, x, swap(y)))
                put(ref, 1, at, jnp.where(lower, swap(x), y))

    def rows_of(load):
        parts = [load(b * lats, 256) for b in range(blocks)]
        parts.append(jnp.concatenate([load(b * lats + 256, HALF) for b in range(blocks)], 0))
        return parts

    def transform(slot, local, even_table, odd_table, cols):
        def project(ref, parts):
            total = None
            for i, part in enumerate(parts):
                term = dot(ref[slot, :, i * 256 : i * 256 + part.shape[0]], part)
                total = term if total is None else total + term
            return total

        results = []
        tables = []
        for c, (ref, load) in enumerate(((even, even_table), (odd, odd_table))):
            parts = rows_of(load)
            tables.append(parts)
            d4 = degree4[local, :, c * half_cols : c * half_cols + cols]
            factor = jnp.where(d4 >= 0.0, 1.0 / (1.0 + rates[...] * d4), 0.0)
            results.append(project(ref, parts) * factor)
        for c, value in enumerate(results):
            for f in range(fld_count):
                for r in range(2):
                    at = (f * 2 + r) * pairs
                    both = jnp.concatenate(
                        [value[at : at + pairs], value[slot_rows + at : slot_rows + at + pairs]], 0
                    )
                    spectra[f, r, local, :, c * half_cols : c * half_cols + cols] = both
                    if cols < half_cols:
                        spectra[f, r, local, :, c * half_cols + cols : (c + 1) * half_cols] = (
                            jnp.zeros((2 * pairs, half_cols - cols), F32)
                        )
        coeff = [v.astype(BF) for v in results]
        for i in range(blocks + 1):
            sym = dot_t(coeff[0], tables[0][i])
            anti = dot_t(coeff[1], tables[1][i])
            at = slice(i * 256, i * 256 + sym.shape[1])
            north[slot, :, at] = (sym + anti).astype(BF)
            south[slot, :, at] = (sym - anti).astype(BF)

    transform(
        2 * pair,
        0,
        lambda at, n: low[0, at : at + n, :half_cols],
        lambda at, n: low[0, at : at + n, half_cols:],
        half_cols,
    )
    transform(
        2 * pair + 1,
        1,
        lambda at, n: jnp.concatenate([h0[0, at : at + n, :], h1[0, at : at + n, :]], 1),
        lambda at, n: jnp.concatenate([h2[0, at : at + n, :], h3[0, at : at + n, :]], 1),
        2 * LANES,
    )

    @pl.when(pair == pl.num_programs(1) - 1)
    def _():
        for block in range(blocks):
            for ref, lat in ((north, block), (south, lat_count - 1 - block)):
                pieces = [
                    get(ref, half, block * 256 + t * LANES) for half in range(2) for t in range(2)
                ]
                at = blocks * 256 + (block // 2) * LANES
                x, y = get(ref, 0, at).astype(F32), get(ref, 1, at).astype(F32)
                rest = jnp.where(lower, x, swap(y)) if block % 2 == 0 else jnp.where(lower, swap(x), y)
                pieces.append(rest.astype(BF))
                if ref is south:
                    pieces = [
                        dot(p, flip_tile if i < 4 else flip_half).astype(BF)
                        for i, p in enumerate(pieces)
                    ]
                joined = dot(scatter[...], jnp.concatenate(pieces, 1)).astype(BF)
                for f in range(fld_count):
                    for k in range(pairs):
                        row = (f * pairs + k) * 2 * GROUP
                        leaving[lat * fld_count + f, :, k * width : (k + 1) * width] = joined[
                            row : row + 2 * GROUP
                        ]


def legendre_step(arrived, tables, own_waves, damp_rates, gauss_weight, lat_count, fld_count):
    slots, half_lats, columns = tables.shape
    half_cols = columns // 2
    sources, _, wide = arrived.shape
    lats = 2 * half_lats // lat_count
    width = 2 * lats
    pairs = wide // width
    slot_rows = 2 * fld_count * pairs
    rows = 2 * slot_rows
    blocks = lat_count // 2
    groups, inner = slots // GROUP, GROUP // 2

    col_index = jnp.arange(columns, dtype=jnp.int32)
    offset = jnp.where(col_index < half_cols, 2 * col_index, 2 * col_index - columns + 1)
    degree = own_waves[:, None] + offset[None, :]
    ratio = (degree * (degree + 1)).astype(F32) / float(LMAX * (LMAX + 1))
    degree4 = jnp.where(degree <= LMAX, ratio**4, -1.0)[:, None, :]

    by_field = damp_rates.reshape(fld_count, 2, pairs)
    rates = jnp.broadcast_to(
        by_field.transpose(1, 0, 2)[:, :, None, :], (2, fld_count, 2, pairs)
    ).reshape(rows, 1)
    w = gauss_weight.reshape(blocks, lats)
    weights = jnp.concatenate([w, w[:, 256:]], 1)

    size = GROUP * slot_rows
    target = jnp.arange(size, dtype=jnp.int32)
    s, rest = target // slot_rows, target % slot_rows
    f, rest = rest // (2 * pairs), rest % (2 * pairs)
    r, k = rest // pairs, rest % pairs
    source = ((f * pairs + k) * GROUP + s) * 2 + r
    gather = (source[:, None] == target[None, :]).astype(BF)
    scatter = (source[None, :] == target[:, None]).astype(BF)
    lane = jnp.arange(LANES, dtype=jnp.int32)
    place = lane[:, None] + lane[None, :]
    same_half = lane[:, None] // HALF == lane[None, :] // HALF
    mirror = jnp.stack(
        [place == LANES - 1, same_half & (place % LANES == HALF - 1)]
    ).astype(BF)

    def slot_of(g, p):
        return g * GROUP + 2 * p

    narrow = [
        pl.BlockSpec((1, half_lats, LANES), functools.partial(lambda t, g, p: (slot_of(g, p) + 1, 0, t), t))
        for t in (0, 1, half_cols // LANES, half_cols // LANES + 1)
    ]
    whole = lambda *shape: pl.BlockSpec(shape, lambda g, p: (0,) * len(shape))
    scratch = pltpu.VMEM((GROUP, rows, half_lats), BF)
    flops = 2 * 2 * slots * rows * half_lats * columns
    return pl.pallas_call(
        functools.partial(legendre_kernel, lat_count, fld_count, lats, half_cols),
        grid=(groups, inner),
        in_specs=[
            pl.BlockSpec((sources, 2 * GROUP, wide), lambda g, p: (0, g, 0)),
            pl.BlockSpec((1, half_lats, columns), lambda g, p: (slot_of(g, p), 0, 0)),
            *narrow,
            pl.BlockSpec((2, 1, columns), lambda g, p: (g * inner + p, 0, 0)),
            whole(rows, 1),
            whole(blocks, 3 * LANES),
            whole(size, size),
            whole(size, size),
            whole(2, LANES, LANES),
        ],
        out_specs=[
            pl.BlockSpec(
                (fld_count, 2, 2, 2 * pairs, columns), lambda g, p: (0, 0, g * inner + p, 0, 0)
            ),
            pl.BlockSpec((sources, 2 * GROUP, wide), lambda g, p: (0, g, 0)),
        ],
        out_shape=[
            jax.ShapeDtypeStruct((fld_count, 2, slots, 2 * pairs, columns), F32),
            jax.ShapeDtypeStruct(arrived.shape, BF),
        ],
        scratch_shapes=[scratch] * 4,
        compiler_params=pltpu.CompilerParams(vmem_limit_bytes=VMEM_BYTES),
        cost_estimate=pl.CostEstimate(
            flops=flops, bytes_accessed=2 * slots * half_lats * columns, transcendentals=0
        ),
        name="legendre",
    )(arrived, tables, *[tables] * 4, degree4, rates, weights, gather, scatter, mirror)


def fast_body(grid_in, legendre, wave_slot, lat_modes, gauss_weight, diffusion):
    fields, lats, lon = grid_in.shape
    slots_all = wave_slot.shape[0]
    lat_count = lax.axis_size("lat")
    fld_count = lax.axis_size("fld")
    owners = lat_count * fld_count
    owned = slots_all // owners
    lat_index = lax.axis_index("lat")
    owner = lat_index * fld_count + lax.axis_index("fld")
    southern = lat_index >= lat_count // 2
    starts = jnp.where(southern, jnp.array([192, 64, 0]), jnp.array([0, 128, 256])).astype(jnp.int32)
    flipped = jnp.concatenate([lat_modes[192:], lat_modes[64:192], lat_modes[:64]])
    ordered = jnp.where(southern, flipped, lat_modes)
    modes = jnp.concatenate([ordered[:256], ordered[:256], ordered[256:], ordered[256:]])[None, :]
    modes = jnp.tile(modes, (1, fields // CHUNKS // 2))
    wave_row = jnp.repeat(wave_slot, 2)[:, None]
    own_waves = lax.dynamic_slice_in_dim(wave_slot, owner * owned, owned)
    rates = diffusion.reshape(fld_count, CHUNKS, fields // CHUNKS)

    def exchange(x):
        return lax.all_to_all(x, ("lat", "fld"), 0, 0, tiled=True)

    angles = angle_rows(wave_row, lon)
    arrived = [
        exchange(dft(grid_in, angles, wave_row, modes, starts, owners, c, CHUNKS))
        for c in range(CHUNKS)
    ]
    parts, back = [], []
    for c in range(CHUNKS):
        part, leaving = legendre_step(
            arrived[c], legendre, own_waves, rates[:, c], gauss_weight, lat_count, fld_count
        )
        parts.append(part)
        back.append(exchange(leaving))
    spectra = share_spectra(jnp.concatenate(parts, 3))
    whole = None
    for c in range(CHUNKS):
        whole = inverse_dft(back[c], angles, wave_row, modes, starts, lats, whole, c, CHUNKS)
    return (whole.reshape(fields, lats, lon), spectra)


def share_spectra(spectra):
    count, parts, slots, fields, columns = spectra.shape
    mine = lax.axis_index("fld")
    result = jnp.zeros((parts, count, slots, fields, columns), F32)
    for shift in range(count):
        block = lax.dynamic_index_in_dim(spectra, (mine + shift) % count, 0, keepdims=False)
        if shift:
            ring = [(i, (i + shift) % count) for i in range(count)]
            block = lax.ppermute(block, "fld", ring)
        at = (mine + count - shift) % count
        result = lax.dynamic_update_slice(result, block[:, None], (0, at, 0, 0, 0))
    return result.reshape(parts, count * slots, fields, columns)


def angle_table(waves, lon_count):
    points = jnp.arange(lon_count, dtype=jnp.int32)
    phase_index = points[:, None] * waves[None, :] % lon_count
    radians = phase_index.astype(jnp.float32) * (2.0 * math.pi / lon_count)
    norm_scale = 1.0 / math.sqrt(lon_count)
    return jnp.stack([jnp.cos(radians) * norm_scale, -jnp.sin(radians) * norm_scale], 1).astype(
        jnp.bfloat16
    )


def damping(waves, damp_rates, columns):
    half_cols = columns // 2
    col_index = jnp.arange(columns, dtype=jnp.int32)
    offset = jnp.where(col_index < half_cols, 2 * col_index, 2 * col_index - columns + 1)
    degree = waves[:, None] + offset[None, :]
    degree_ratio = (degree * (degree + 1)).astype(jnp.float32) / float(LMAX * (LMAX + 1))
    factor = 1.0 / (1.0 + damp_rates[None, :, None] * (degree_ratio**4)[:, None, :])
    return jnp.where((degree <= LMAX)[:, None, :], factor, 0.0)


def project(even_part, odd_part, tables, used_cols):
    half_cols = tables.shape[2] // 2
    even_cols = jnp.einsum(
        "rsfj,sjq->rsfq", even_part, tables[:, :, :used_cols], preferred_element_type=jnp.float32
    )
    odd_cols = jnp.einsum(
        "rsfj,sjq->rsfq",
        odd_part,
        tables[:, :, half_cols : half_cols + used_cols],
        preferred_element_type=jnp.float32,
    )
    return jnp.concatenate([even_cols, odd_cols], -1)


def expand(rounded, tables, used_cols):
    half_cols = tables.shape[2] // 2
    sym_part = jnp.einsum(
        "rsfq,sjq->rsfj",
        rounded[..., :used_cols],
        tables[:, :, :used_cols],
        preferred_element_type=jnp.float32,
    )
    anti_part = jnp.einsum(
        "rsfq,sjq->rsfj",
        rounded[..., half_cols : half_cols + used_cols],
        tables[:, :, half_cols : half_cols + used_cols],
        preferred_element_type=jnp.float32,
    )
    return (sym_part, anti_part)


def transform_block(block_data, tables, block_waves, damp_rates, weights):
    half_lats = weights.shape[0]
    columns = tables.shape[2]
    half_cols = columns // 2
    north_half = block_data[..., :half_lats].astype(jnp.float32)
    south_half = jnp.flip(block_data[..., half_lats:], -1).astype(jnp.float32)
    even_part = ((north_half + south_half) * weights).astype(jnp.bfloat16)
    odd_part = ((north_half - south_half) * weights).astype(jnp.bfloat16)
    raw_coeff = project(even_part, odd_part, tables, half_cols)
    spectra = raw_coeff * damping(block_waves, damp_rates, columns)[None]
    rounded = spectra.astype(jnp.bfloat16)
    sym_part, anti_part = expand(rounded, tables, half_cols)
    synthesized = jnp.concatenate(
        [
            (sym_part + anti_part).astype(jnp.bfloat16),
            jnp.flip((sym_part - anti_part).astype(jnp.bfloat16), -1),
        ],
        -1,
    )
    return (spectra, synthesized)


def general_body(grid_in, legendre, wave_slot, lat_modes, gauss_weight, diffusion):
    fld_dev, lat_dev, lon_count = grid_in.shape
    slots_all = wave_slot.shape[0]
    lat_count = lax.axis_size("lat")
    fld_count = lax.axis_size("fld")
    lat_total = lat_dev * lat_count
    lat_index = lax.axis_index("lat")
    fld_index = lax.axis_index("fld")
    owned_slots = slots_all // (lat_count * fld_count)
    angles = angle_table(wave_slot, lon_count)
    keep_mask = (wave_slot[:, None] < lat_modes[None, :]).astype(jnp.float32)
    fourier = jnp.einsum("fjx,xrs->rsfj", grid_in, angles, preferred_element_type=jnp.float32)
    fourier = (fourier * keep_mask[None, :, None, :]).astype(jnp.bfloat16)
    own_waves = lax.dynamic_slice_in_dim(
        wave_slot, (lat_index * fld_count + fld_index) * owned_slots, owned_slots
    )
    flattened = fourier.reshape(2, slots_all, fld_dev * lat_dev)
    arrived = lax.all_to_all(flattened, ("lat", "fld"), split_axis=1, concat_axis=2, tiled=True)
    arrived = arrived.reshape(2, owned_slots, lat_count, fld_count, fld_dev, lat_dev)
    arrived = arrived.transpose(0, 1, 3, 4, 2, 5).reshape(
        2, owned_slots, fld_count * fld_dev, lat_total
    )
    owned_spectra, synthesized = transform_block(
        arrived, legendre, own_waves, diffusion, gauss_weight
    )
    spectra = lax.all_to_all(owned_spectra, "fld", split_axis=2, concat_axis=1, tiled=True)
    outgoing = synthesized.reshape(2, owned_slots, fld_count, fld_dev, lat_count, lat_dev)
    outgoing = outgoing.transpose(0, 1, 4, 2, 3, 5).reshape(
        2, owned_slots, lat_count * fld_count * fld_dev * lat_dev
    )
    returned = lax.all_to_all(outgoing, ("lat", "fld"), split_axis=2, concat_axis=1, tiled=True)
    returned = returned.reshape(2, slots_all, fld_dev, lat_dev)
    keep_narrow = keep_mask.astype(jnp.bfloat16)
    masked = returned * keep_narrow[None, :, None, :]
    grid_out = 2.0 * jnp.einsum("rsfj,xrs->fjx", masked, angles, preferred_element_type=jnp.float32)
    return (grid_out, spectra)


def body(grid_in, legendre, wave_slot, lat_modes, gauss_weight, diffusion):
    fields, lats, lon = grid_in.shape
    slots, _, columns = legendre.shape
    lat_count = lax.axis_size("lat")
    fits = (
        lats == 2 * LANES + HALF
        and lat_count % 4 == 0
        and fields % (2 * CHUNKS) == 0
        and lat_count * lax.axis_size("fld") % 8 == 0
        and slots % GROUP == 0
        and lon % LANES == 0 and lon % 4 == 0
        and columns == 6 * LANES
    )
    chosen = fast_body if fits else general_body
    return chosen(grid_in, legendre, wave_slot, lat_modes, gauss_weight, diffusion)


def solution(mesh):
    return jax.shard_map(
        body,
        mesh=mesh,
        in_specs=(P("fld", "lat", None), P(("lat", "fld"), None, None), P(), P("lat"), P(), P()),
        out_specs=(P("fld", "lat", None), P(None, "lat", "fld", None)),
        check_vma=False,
    )
```

```python
import functools
import math

import jax
import jax.numpy as jnp
from jax import lax
from jax.experimental import pallas as pl
from jax.experimental.pallas import tpu as pltpu
from jax.sharding import PartitionSpec as P

LMAX = 1279
LANES = 128
HALF = 64
GROUP = 8
CHUNKS = 2
BF = jnp.bfloat16
F32 = jnp.float32
VMEM_BYTES = 60 * 1024 * 1024
INVERSE_VMEM_BYTES = 44 * 1024 * 1024


def dot(a, b):
    return jnp.dot(a, b, preferred_element_type=F32)


def dot_t(a, b):
    return lax.dot_general(a, b, (((1,), (1,)), ((), ())), preferred_element_type=F32)


def turn_cos(phase, count):
    whole = phase - jnp.floor(phase * (1.0 / count) + 0.5) * count
    x = whole * (2.0 * math.pi / count)
    square = x * x
    total = jnp.full_like(square, 1.0 / math.factorial(18) * -1.0)
    for order in range(16, -1, -2):
        total = total * square + (-1.0) ** (order // 2) / math.factorial(order)
    return total


def angle_kernel(lon, wave_row, out):
    rows = out.shape[0]
    step = 64
    scale = 1.0 / math.sqrt(lon)
    tiles = lon // LANES
    restart = (tiles + 1) // 2

    @pl.loop(0, rows // step)
    def _(i):
        at = pl.ds(pl.multiple_of(i * step, step), step)
        wave = jnp.broadcast_to(wave_row[at, :].astype(F32), (step, LANES))
        lane = lax.broadcasted_iota(jnp.int32, (step, LANES), 1).astype(F32)
        part = lax.broadcasted_iota(jnp.int32, (step, LANES), 0)
        turn = (part % 2 * (lon // 4)).astype(F32)
        fine = wave * lane + turn
        coarse = wave * LANES
        double = 2.0 * turn_cos(coarse, lon)
        for a in range(tiles):
            if a % restart == 0:
                before = turn_cos(fine + coarse * (a - 1), lon) * scale
                value = turn_cos(fine + coarse * a, lon) * scale
            else:
                before, value = value, double * value - before
            out[at, a * LANES : (a + 1) * LANES] = value.astype(BF)


def angle_rows(wave_row, lon):
    rows = wave_row.shape[0]
    step = 256
    return pl.pallas_call(
        functools.partial(angle_kernel, lon),
        grid=(rows // step,),
        in_specs=[pl.BlockSpec((step, 1), lambda i: (i, 0))],
        out_specs=pl.BlockSpec((step, lon), lambda i: (i, 0)),
        out_shape=jax.ShapeDtypeStruct((rows, lon), BF),
        cost_estimate=pl.CostEstimate(
            flops=4 * rows * lon, bytes_accessed=2 * rows * lon, transcendentals=0
        ),
        name="angles",
    )(wave_row)


def dft_kernel(count, starts, *refs):
    fields = refs[:count]
    angles, wave_row, modes, out, arranged = refs[count:]
    pairs = count // 2
    width = out.shape[2] // pairs

    @pl.when(pl.program_id(0) == 0)
    def _():
        first, second, rest = (pl.multiple_of(starts[i], HALF) for i in range(3))
        for i, field in enumerate(fields):
            half, pair = divmod(i, pairs)
            at = pair * width + half * 256
            arranged[at : at + 128] = field[0, pl.ds(first, 128), :]
            arranged[at + 128 : at + 256] = field[0, pl.ds(second, 128), :]
            at = pair * width + 512 + half * HALF
            arranged[at : at + HALF] = field[0, pl.ds(rest, HALF), :]

    value = dot_t(angles[...], arranged[...])
    value = jnp.where(wave_row[...] < modes[...], value, 0.0)
    out[...] = value.astype(BF).reshape(out.shape)


def dft(grid_in, angles, wave_row, modes, starts, dests, chunk, chunks):
    fields, lats, lon = grid_in.shape
    count = fields // chunks
    rows = angles.shape[0]
    wide = count * lats
    per = dests // 2
    tile = rows * per // dests
    return pl.pallas_call(
        functools.partial(dft_kernel, count),
        grid_spec=pltpu.PrefetchScalarGridSpec(
            num_scalar_prefetch=1,
            grid=(dests // per,),
            in_specs=[
                *[
                    pl.BlockSpec(
                        (1, lats, lon), functools.partial(lambda f, i, s: (f, 0, 0), chunk * count + f)
                    )
                    for f in range(count)
                ],
                pl.BlockSpec((tile, lon), lambda i, s: (i, 0)),
                pl.BlockSpec((tile, 1), lambda i, s: (i, 0)),
                pl.BlockSpec((1, wide), lambda i, s: (0, 0)),
            ],
            out_specs=pl.BlockSpec((per, rows // dests, wide), lambda i, s: (i, 0, 0)),
            scratch_shapes=[pltpu.VMEM((wide, lon), BF)],
        ),
        out_shape=jax.ShapeDtypeStruct((dests, rows // dests, wide), BF),
        compiler_params=pltpu.CompilerParams(vmem_limit_bytes=VMEM_BYTES),
        cost_estimate=pl.CostEstimate(
            flops=2 * rows * wide * lon, bytes_accessed=2 * wide * (lon + rows), transcendentals=0
        ),
        name="dft",
    )(starts, *[grid_in] * count, angles, wave_row, modes)


def inverse_kernel(starts, back, angles, wave_row, modes, *refs):
    out, turned = refs[-2:]
    first, second, rest = (pl.multiple_of(starts[i], HALF) for i in range(3))
    dests, rows, width = back.shape
    per = 8
    count = per * rows
    for i in range(dests // per):
        value = back[i * per : (i + 1) * per].reshape(count, width).astype(F32)
        value = jnp.where(wave_row[i * count : (i + 1) * count, :] < modes[...], value, 0.0)
        turned[:, i * count : (i + 1) * count] = value.T.astype(BF)
    lon = angles.shape[1]
    step = 6 * LANES
    for at in range(0, lon, step):
        cols = slice(at, min(at + step, lon))
        value = 2.0 * dot(turned[...], angles[:, cols])
        for i in range(2):
            out[0, i, 0, pl.ds(first, 128), cols] = value[i * 256 : i * 256 + 128]
            out[0, i, 0, pl.ds(second, 128), cols] = value[i * 256 + 128 : i * 256 + 256]
            out[0, i, 0, pl.ds(rest, HALF), cols] = value[512 + i * HALF : 512 + (i + 1) * HALF]


def inverse_dft(back, angles, wave_row, modes, starts, lats, whole, chunk, chunks):
    dests, rows, wide = back.shape
    lon = angles.shape[1]
    width = 2 * lats
    pairs = wide // width
    given = [] if whole is None else [whole]
    return pl.pallas_call(
        inverse_kernel,
        grid_spec=pltpu.PrefetchScalarGridSpec(
            num_scalar_prefetch=1,
            grid=(pairs,),
            in_specs=[
                pl.BlockSpec((dests, rows, width), lambda k, s: (0, 0, k)),
                pl.BlockSpec(memory_space=pltpu.VMEM),
                pl.BlockSpec((dests * rows, 1), lambda k, s: (0, 0)),
                pl.BlockSpec((1, width), lambda k, s: (0, 0)),
                *[pl.BlockSpec(memory_space=pl.ANY) for _ in given],
            ],
            out_specs=pl.BlockSpec((1, 2, 1, lats, lon), lambda k, s: (chunk, 0, k, 0, 0)),
            scratch_shapes=[pltpu.VMEM((width, dests * rows), BF)],
        ),
        out_shape=jax.ShapeDtypeStruct((chunks, 2, pairs, lats, lon), F32),
        input_output_aliases={5: 0} if given else {},
        compiler_params=pltpu.CompilerParams(vmem_limit_bytes=INVERSE_VMEM_BYTES),
        cost_estimate=pl.CostEstimate(
            flops=2 * dests * rows * wide * lon,
            bytes_accessed=wide * (4 * lon + 2 * dests * rows),
            transcendentals=0,
        ),
        name="inverse_dft",
    )(starts, back, angles, wave_row, modes[:, :width], *given)


def legendre_kernel(
    lat_count,
    fld_count,
    lats,
    half_cols,
    arrived,
    low,
    h0,
    h1,
    h2,
    h3,
    degree4,
    rates,
    weights,
    gather,
    scatter,
    mirror,
    spectra,
    leaving,
    even,
    odd,
    north,
    south,
):
    pair = pl.program_id(1)
    blocks = lat_count // 2
    width = 2 * lats
    pairs = arrived.shape[2] // width
    slot_rows = 2 * fld_count * pairs
    lower = lax.broadcasted_iota(jnp.int32, (GROUP * slot_rows, LANES), 1) < HALF
    flip_tile = mirror[0]
    flip_half = mirror[1]

    def swap(x):
        return pltpu.roll(x, HALF, 1)

    def put(ref, half, at, x):
        ref[:, half * slot_rows : (half + 1) * slot_rows, at : at + LANES] = x.astype(BF).reshape(
            GROUP, slot_rows, LANES
        )

    def get(ref, half, at):
        return ref[:, half * slot_rows : (half + 1) * slot_rows, at : at + LANES].reshape(
            GROUP * slot_rows, LANES
        )

    def stacked(lat):
        parts = [
            arrived[lat * fld_count + f, :, k * width : (k + 1) * width]
            for f in range(fld_count)
            for k in range(pairs)
        ]
        return dot(gather[...], jnp.concatenate(parts, 0))

    @pl.when(pair == 0)
    def _():
        rests = []
        for block in range(blocks):
            up = stacked(block)
            down = stacked(lat_count - 1 - block).astype(BF)
            for piece in range(5):
                tile = slice(piece * LANES, (piece + 1) * LANES)
                n = up[:, tile]
                s = dot(down[:, tile], flip_tile if piece < 4 else flip_half)
                w = weights[block : block + 1, 2 * LANES :] if piece == 4 else (
                    weights[block : block + 1, (piece % 2) * LANES : (piece % 2 + 1) * LANES]
                )
                e, o = (n + s) * w, (n - s) * w
                if piece < 4:
                    at = block * 256 + (piece % 2) * LANES
                    put(even, piece // 2, at, e)
                    put(odd, piece // 2, at, o)
                else:
                    rests.append((e, o))
        for b in range(blocks // 2):
            at = blocks * 256 + b * LANES
            for ref, c in ((even, 0), (odd, 1)):
                x, y = rests[2 * b][c], rests[2 * b + 1][c]
                put(ref, 0, at, jnp.where(lower, x, swap(y)))
                put(ref, 1, at, jnp.where(lower, swap(x), y))

    def rows_of(load):
        parts = [load(b * lats, 256) for b in range(blocks)]
        parts.append(jnp.concatenate([load(b * lats + 256, HALF) for b in range(blocks)], 0))
        return parts

    def transform(slot, local, even_table, odd_table, cols):
        def project(ref, parts):
            total = None
            for i, part in enumerate(parts):
                term = dot(ref[slot, :, i * 256 : i * 256 + part.shape[0]], part)
                total = term if total is None else total + term
            return total

        results = []
        tables = []
        for c, (ref, load) in enumerate(((even, even_table), (odd, odd_table))):
            parts = rows_of(load)
            tables.append(parts)
            d4 = degree4[local, :, c * half_cols : c * half_cols + cols]
            factor = jnp.where(d4 >= 0.0, 1.0 / (1.0 + rates[...] * d4), 0.0)
            results.append(project(ref, parts) * factor)
        for c, value in enumerate(results):
            for f in range(fld_count):
                for r in range(2):
                    at = (f * 2 + r) * pairs
                    both = jnp.concatenate(
                        [value[at : at + pairs], value[slot_rows + at : slot_rows + at + pairs]], 0
                    )
                    spectra[f, r, local, :, c * half_cols : c * half_cols + cols] = both
                    if cols < half_cols:
                        spectra[f, r, local, :, c * half_cols + cols : (c + 1) * half_cols] = (
                            jnp.zeros((2 * pairs, half_cols - cols), F32)
                        )
        coeff = [v.astype(BF) for v in results]
        for i in range(blocks + 1):
            sym = dot_t(coeff[0], tables[0][i])
            anti = dot_t(coeff[1], tables[1][i])
            at = slice(i * 256, i * 256 + sym.shape[1])
            north[slot, :, at] = (sym + anti).astype(BF)
            south[slot, :, at] = (sym - anti).astype(BF)

    transform(
        2 * pair,
        0,
        lambda at, n: low[0, at : at + n, :half_cols],
        lambda at, n: low[0, at : at + n, half_cols:],
        half_cols,
    )
    transform(
        2 * pair + 1,
        1,
        lambda at, n: jnp.concatenate([h0[0, at : at + n, :], h1[0, at : at + n, :]], 1),
        lambda at, n: jnp.concatenate([h2[0, at : at + n, :], h3[0, at : at + n, :]], 1),
        2 * LANES,
    )

    @pl.when(pair == pl.num_programs(1) - 1)
    def _():
        for block in range(blocks):
            for ref, lat in ((north, block), (south, lat_count - 1 - block)):
                pieces = [
                    get(ref, half, block * 256 + t * LANES) for half in range(2) for t in range(2)
                ]
                at = blocks * 256 + (block // 2) * LANES
                x, y = get(ref, 0, at).astype(F32), get(ref, 1, at).astype(F32)
                rest = jnp.where(lower, x, swap(y)) if block % 2 == 0 else jnp.where(lower, swap(x), y)
                pieces.append(rest.astype(BF))
                if ref is south:
                    pieces = [
                        dot(p, flip_tile if i < 4 else flip_half).astype(BF)
                        for i, p in enumerate(pieces)
                    ]
                joined = dot(scatter[...], jnp.concatenate(pieces, 1)).astype(BF)
                for f in range(fld_count):
                    for k in range(pairs):
                        row = (f * pairs + k) * 2 * GROUP
                        leaving[lat * fld_count + f, :, k * width : (k + 1) * width] = joined[
                            row : row + 2 * GROUP
                        ]


def legendre_step(arrived, tables, own_waves, damp_rates, gauss_weight, lat_count, fld_count):
    slots, half_lats, columns = tables.shape
    half_cols = columns // 2
    sources, _, wide = arrived.shape
    lats = 2 * half_lats // lat_count
    width = 2 * lats
    pairs = wide // width
    slot_rows = 2 * fld_count * pairs
    rows = 2 * slot_rows
    blocks = lat_count // 2
    groups, inner = slots // GROUP, GROUP // 2

    col_index = jnp.arange(columns, dtype=jnp.int32)
    offset = jnp.where(col_index < half_cols, 2 * col_index, 2 * col_index - columns + 1)
    degree = own_waves[:, None] + offset[None, :]
    ratio = (degree * (degree + 1)).astype(F32) / float(LMAX * (LMAX + 1))
    degree4 = jnp.where(degree <= LMAX, ratio**4, -1.0)[:, None, :]

    by_field = damp_rates.reshape(fld_count, 2, pairs)
    rates = jnp.broadcast_to(
        by_field.transpose(1, 0, 2)[:, :, None, :], (2, fld_count, 2, pairs)
    ).reshape(rows, 1)
    w = gauss_weight.reshape(blocks, lats)
    weights = jnp.concatenate([w, w[:, 256:]], 1)

    size = GROUP * slot_rows
    target = jnp.arange(size, dtype=jnp.int32)
    s, rest = target // slot_rows, target % slot_rows
    f, rest = rest // (2 * pairs), rest % (2 * pairs)
    r, k = rest // pairs, rest % pairs
    source = ((f * pairs + k) * GROUP + s) * 2 + r
    gather = (source[:, None] == target[None, :]).astype(BF)
    scatter = (source[None, :] == target[:, None]).astype(BF)
    lane = jnp.arange(LANES, dtype=jnp.int32)
    place = lane[:, None] + lane[None, :]
    same_half = lane[:, None] // HALF == lane[None, :] // HALF
    mirror = jnp.stack(
        [place == LANES - 1, same_half & (place % LANES == HALF - 1)]
    ).astype(BF)

    def slot_of(g, p):
        return g * GROUP + 2 * p

    narrow = [
        pl.BlockSpec((1, half_lats, LANES), functools.partial(lambda t, g, p: (slot_of(g, p) + 1, 0, t), t))
        for t in (0, 1, half_cols // LANES, half_cols // LANES + 1)
    ]
    whole = lambda *shape: pl.BlockSpec(shape, lambda g, p: (0,) * len(shape))
    scratch = pltpu.VMEM((GROUP, rows, half_lats), BF)
    flops = 2 * 2 * slots * rows * half_lats * columns
    return pl.pallas_call(
        functools.partial(legendre_kernel, lat_count, fld_count, lats, half_cols),
        grid=(groups, inner),
        in_specs=[
            pl.BlockSpec((sources, 2 * GROUP, wide), lambda g, p: (0, g, 0)),
            pl.BlockSpec((1, half_lats, columns), lambda g, p: (slot_of(g, p), 0, 0)),
            *narrow,
            pl.BlockSpec((2, 1, columns), lambda g, p: (g * inner + p, 0, 0)),
            whole(rows, 1),
            whole(blocks, 3 * LANES),
            whole(size, size),
            whole(size, size),
            whole(2, LANES, LANES),
        ],
        out_specs=[
            pl.BlockSpec(
                (fld_count, 2, 2, 2 * pairs, columns), lambda g, p: (0, 0, g * inner + p, 0, 0)
            ),
            pl.BlockSpec((sources, 2 * GROUP, wide), lambda g, p: (0, g, 0)),
        ],
        out_shape=[
            jax.ShapeDtypeStruct((fld_count, 2, slots, 2 * pairs, columns), F32),
            jax.ShapeDtypeStruct(arrived.shape, BF),
        ],
        scratch_shapes=[scratch] * 4,
        compiler_params=pltpu.CompilerParams(vmem_limit_bytes=VMEM_BYTES),
        cost_estimate=pl.CostEstimate(
            flops=flops, bytes_accessed=2 * slots * half_lats * columns, transcendentals=0
        ),
        name="legendre",
    )(arrived, tables, *[tables] * 4, degree4, rates, weights, gather, scatter, mirror)


def fast_body(grid_in, legendre, wave_slot, lat_modes, gauss_weight, diffusion):
    fields, lats, lon = grid_in.shape
    slots_all = wave_slot.shape[0]
    lat_count = lax.axis_size("lat")
    fld_count = lax.axis_size("fld")
    owners = lat_count * fld_count
    owned = slots_all // owners
    lat_index = lax.axis_index("lat")
    owner = lat_index * fld_count + lax.axis_index("fld")
    southern = lat_index >= lat_count // 2
    starts = jnp.where(southern, jnp.array([192, 64, 0]), jnp.array([0, 128, 256])).astype(jnp.int32)
    flipped = jnp.concatenate([lat_modes[192:], lat_modes[64:192], lat_modes[:64]])
    ordered = jnp.where(southern, flipped, lat_modes)
    modes = jnp.concatenate([ordered[:256], ordered[:256], ordered[256:], ordered[256:]])[None, :]
    modes = jnp.tile(modes, (1, fields // CHUNKS // 2))
    wave_row = jnp.repeat(wave_slot, 2)[:, None]
    own_waves = lax.dynamic_slice_in_dim(wave_slot, owner * owned, owned)
    rates = diffusion.reshape(fld_count, CHUNKS, fields // CHUNKS)

    def exchange(x):
        return lax.all_to_all(x, ("lat", "fld"), 0, 0, tiled=True)

    angles = angle_rows(wave_row, lon)
    arrived = [
        exchange(dft(grid_in, angles, wave_row, modes, starts, owners, c, CHUNKS))
        for c in range(CHUNKS)
    ]
    parts, back = [], []
    for c in range(CHUNKS):
        part, leaving = legendre_step(
            arrived[c], legendre, own_waves, rates[:, c], gauss_weight, lat_count, fld_count
        )
        if parts:
            places, blocks = zip(*parts[-1])
            leaving, blocks = lax.optimization_barrier((leaving, blocks))
            parts[-1] = list(zip(places, blocks))
        back.append(exchange(leaving))
        parts.append(share_spectra(part))
    whole = None
    columns = legendre.shape[2]
    spectra = jnp.zeros((2, fld_count, owned, fields, columns), F32)
    for c in range(CHUNKS):
        whole = inverse_dft(back[c], angles, wave_row, modes, starts, lats, whole, c, CHUNKS)
        if c == 0:
            whole, spectra = lax.optimization_barrier((whole, spectra))
    for c in range(CHUNKS):
        for at, block in parts[c]:
            spectra = lax.dynamic_update_slice(
                spectra, block[:, None], (0, at, 0, c * (fields // CHUNKS), 0)
            )
    return (whole.reshape(fields, lats, lon), spectra.reshape(2, -1, fields, columns))


def share_spectra(part):
    count = part.shape[0]
    mine = lax.axis_index("fld")
    blocks = []
    for shift in range(count):
        block = lax.dynamic_index_in_dim(part, (mine + shift) % count, 0, keepdims=False)
        if shift:
            ring = [(i, (i + shift) % count) for i in range(count)]
            block = lax.ppermute(block, "fld", ring)
        blocks.append(((mine + count - shift) % count, block))
    return blocks


def angle_table(waves, lon_count):
    points = jnp.arange(lon_count, dtype=jnp.int32)
    phase_index = points[:, None] * waves[None, :] % lon_count
    radians = phase_index.astype(jnp.float32) * (2.0 * math.pi / lon_count)
    norm_scale = 1.0 / math.sqrt(lon_count)
    return jnp.stack([jnp.cos(radians) * norm_scale, -jnp.sin(radians) * norm_scale], 1).astype(
        jnp.bfloat16
    )


def damping(waves, damp_rates, columns):
    half_cols = columns // 2
    col_index = jnp.arange(columns, dtype=jnp.int32)
    offset = jnp.where(col_index < half_cols, 2 * col_index, 2 * col_index - columns + 1)
    degree = waves[:, None] + offset[None, :]
    degree_ratio = (degree * (degree + 1)).astype(jnp.float32) / float(LMAX * (LMAX + 1))
    factor = 1.0 / (1.0 + damp_rates[None, :, None] * (degree_ratio**4)[:, None, :])
    return jnp.where((degree <= LMAX)[:, None, :], factor, 0.0)


def project(even_part, odd_part, tables, used_cols):
    half_cols = tables.shape[2] // 2
    even_cols = jnp.einsum(
        "rsfj,sjq->rsfq", even_part, tables[:, :, :used_cols], preferred_element_type=jnp.float32
    )
    odd_cols = jnp.einsum(
        "rsfj,sjq->rsfq",
        odd_part,
        tables[:, :, half_cols : half_cols + used_cols],
        preferred_element_type=jnp.float32,
    )
    return jnp.concatenate([even_cols, odd_cols], -1)


def expand(rounded, tables, used_cols):
    half_cols = tables.shape[2] // 2
    sym_part = jnp.einsum(
        "rsfq,sjq->rsfj",
        rounded[..., :used_cols],
        tables[:, :, :used_cols],
        preferred_element_type=jnp.float32,
    )
    anti_part = jnp.einsum(
        "rsfq,sjq->rsfj",
        rounded[..., half_cols : half_cols + used_cols],
        tables[:, :, half_cols : half_cols + used_cols],
        preferred_element_type=jnp.float32,
    )
    return (sym_part, anti_part)


def transform_block(block_data, tables, block_waves, damp_rates, weights):
    half_lats = weights.shape[0]
    columns = tables.shape[2]
    half_cols = columns // 2
    north_half = block_data[..., :half_lats].astype(jnp.float32)
    south_half = jnp.flip(block_data[..., half_lats:], -1).astype(jnp.float32)
    even_part = ((north_half + south_half) * weights).astype(jnp.bfloat16)
    odd_part = ((north_half - south_half) * weights).astype(jnp.bfloat16)
    raw_coeff = project(even_part, odd_part, tables, half_cols)
    spectra = raw_coeff * damping(block_waves, damp_rates, columns)[None]
    rounded = spectra.astype(jnp.bfloat16)
    sym_part, anti_part = expand(rounded, tables, half_cols)
    synthesized = jnp.concatenate(
        [
            (sym_part + anti_part).astype(jnp.bfloat16),
            jnp.flip((sym_part - anti_part).astype(jnp.bfloat16), -1),
        ],
        -1,
    )
    return (spectra, synthesized)


def general_body(grid_in, legendre, wave_slot, lat_modes, gauss_weight, diffusion):
    fld_dev, lat_dev, lon_count = grid_in.shape
    slots_all = wave_slot.shape[0]
    lat_count = lax.axis_size("lat")
    fld_count = lax.axis_size("fld")
    lat_total = lat_dev * lat_count
    lat_index = lax.axis_index("lat")
    fld_index = lax.axis_index("fld")
    owned_slots = slots_all // (lat_count * fld_count)
    angles = angle_table(wave_slot, lon_count)
    keep_mask = (wave_slot[:, None] < lat_modes[None, :]).astype(jnp.float32)
    fourier = jnp.einsum("fjx,xrs->rsfj", grid_in, angles, preferred_element_type=jnp.float32)
    fourier = (fourier * keep_mask[None, :, None, :]).astype(jnp.bfloat16)
    own_waves = lax.dynamic_slice_in_dim(
        wave_slot, (lat_index * fld_count + fld_index) * owned_slots, owned_slots
    )
    flattened = fourier.reshape(2, slots_all, fld_dev * lat_dev)
    arrived = lax.all_to_all(flattened, ("lat", "fld"), split_axis=1, concat_axis=2, tiled=True)
    arrived = arrived.reshape(2, owned_slots, lat_count, fld_count, fld_dev, lat_dev)
    arrived = arrived.transpose(0, 1, 3, 4, 2, 5).reshape(
        2, owned_slots, fld_count * fld_dev, lat_total
    )
    owned_spectra, synthesized = transform_block(
        arrived, legendre, own_waves, diffusion, gauss_weight
    )
    spectra = lax.all_to_all(owned_spectra, "fld", split_axis=2, concat_axis=1, tiled=True)
    outgoing = synthesized.reshape(2, owned_slots, fld_count, fld_dev, lat_count, lat_dev)
    outgoing = outgoing.transpose(0, 1, 4, 2, 3, 5).reshape(
        2, owned_slots, lat_count * fld_count * fld_dev * lat_dev
    )
    returned = lax.all_to_all(outgoing, ("lat", "fld"), split_axis=2, concat_axis=1, tiled=True)
    returned = returned.reshape(2, slots_all, fld_dev, lat_dev)
    keep_narrow = keep_mask.astype(jnp.bfloat16)
    masked = returned * keep_narrow[None, :, None, :]
    grid_out = 2.0 * jnp.einsum("rsfj,xrs->fjx", masked, angles, preferred_element_type=jnp.float32)
    return (grid_out, spectra)


def body(grid_in, legendre, wave_slot, lat_modes, gauss_weight, diffusion):
    fields, lats, lon = grid_in.shape
    slots, _, columns = legendre.shape
    lat_count = lax.axis_size("lat")
    fits = (
        lats == 2 * LANES + HALF
        and lat_count % 4 == 0
        and fields % (2 * CHUNKS) == 0
        and lat_count * lax.axis_size("fld") % 8 == 0
        and slots % GROUP == 0
        and lon % LANES == 0 and lon % 4 == 0
        and columns == 6 * LANES
    )
    chosen = fast_body if fits else general_body
    return chosen(grid_in, legendre, wave_slot, lat_modes, gauss_weight, diffusion)


def solution(mesh):
    return jax.shard_map(
        body,
        mesh=mesh,
        in_specs=(P("fld", "lat", None), P(("lat", "fld"), None, None), P(), P("lat"), P(), P()),
        out_specs=(P("fld", "lat", None), P(None, "lat", "fld", None)),
        check_vma=False,
    )
```

```python
import functools
import math

import jax
import jax.numpy as jnp
from jax import lax
from jax.experimental import pallas as pl
from jax.experimental.pallas import tpu as pltpu
from jax.sharding import PartitionSpec as P

LMAX = 1279
LANES = 128
HALF = 64
GROUP = 8
OUTWARD = ((2,), (0, 1, 3))
RETURN = ((2,), (0, 1), (3,))
BF = jnp.bfloat16
F32 = jnp.float32
VMEM_BYTES = 60 * 1024 * 1024


def dot(a, b):
    return jnp.dot(a, b, preferred_element_type=F32)


def dot_t(a, b):
    return lax.dot_general(a, b, (((1,), (1,)), ((), ())), preferred_element_type=F32)


def turn_cos(phase, count):
    whole = phase - jnp.floor(phase * (1.0 / count) + 0.5) * count
    half = whole * (math.pi / count)
    square = half * half
    total = jnp.full_like(square, -1.0 / math.factorial(14))
    for order in range(12, -1, -2):
        total = total * square + (-1.0) ** (order // 2) / math.factorial(order)
    return 2.0 * (total * total) - 1.0


def angle_kernel(lon, wave_row, out):
    rows = out.shape[0]
    step = 64
    scale = 1.0 / math.sqrt(lon)
    tiles = lon // LANES
    middle = tiles // 2

    @pl.loop(0, rows // step)
    def _(i):
        at = pl.ds(pl.multiple_of(i * step, step), step)
        wave = jnp.broadcast_to(wave_row[at, :].astype(F32), (step, LANES))
        lane = lax.broadcasted_iota(jnp.int32, (step, LANES), 1).astype(F32)
        part = lax.broadcasted_iota(jnp.int32, (step, LANES), 0)
        turn = (part % 2 * (lon // 4)).astype(F32)
        fine = wave * lane + turn
        coarse = wave * LANES
        double = 2.0 * turn_cos(coarse, lon)
        pair = [turn_cos(fine + coarse * a, lon) * scale for a in (middle, middle + 1)]

        def put(a, x):
            out[at, a * LANES : (a + 1) * LANES] = x.astype(BF)

        put(middle, pair[0])
        put(middle + 1, pair[1])
        before, value = pair
        for a in range(middle + 2, tiles):
            before, value = value, double * value - before
            put(a, value)
        value, before = pair
        for a in range(middle - 1, -1, -1):
            before, value = value, double * value - before
            put(a, value)


def angle_rows(wave_row, lon):
    rows = wave_row.shape[0]
    step = 256
    return pl.pallas_call(
        functools.partial(angle_kernel, lon),
        grid=(rows // step,),
        in_specs=[pl.BlockSpec((step, 1), lambda i: (i, 0))],
        out_specs=pl.BlockSpec((step, lon), lambda i: (i, 0)),
        out_shape=jax.ShapeDtypeStruct((rows, lon), BF),
        cost_estimate=pl.CostEstimate(
            flops=4 * rows * lon, bytes_accessed=2 * rows * lon, transcendentals=0
        ),
        name="angles",
    )(wave_row)


def dft_kernel(count, starts, *refs):
    fields = refs[:count]
    angles, wave_row, modes, out, arranged = refs[count:]
    width = out.shape[2] // (count // 2)

    @pl.when(pl.program_id(0) == 0)
    def _():
        first, second, rest = (pl.multiple_of(starts[i], HALF) for i in range(3))
        for i, field in enumerate(fields):
            pair, half = divmod(i, 2)
            at = pair * width + half * 256
            arranged[at : at + 128] = field[0, pl.ds(first, 128), :]
            arranged[at + 128 : at + 256] = field[0, pl.ds(second, 128), :]
            at = pair * width + 512 + half * HALF
            arranged[at : at + HALF] = field[0, pl.ds(rest, HALF), :]

    value = dot_t(angles[...], arranged[...])
    value = jnp.where(wave_row[...] < modes[...], value, 0.0)
    out[...] = value.astype(BF).reshape(out.shape)


def dft(grid_in, angles, wave_row, modes, starts, dests, pairs):
    _, lats, lon = grid_in.shape
    count = 2 * len(pairs)
    rows = angles.shape[0]
    wide = count * lats
    per = dests // 4
    tile = rows * per // dests
    return pl.pallas_call(
        functools.partial(dft_kernel, count),
        grid_spec=pltpu.PrefetchScalarGridSpec(
            num_scalar_prefetch=1,
            grid=(dests // per,),
            in_specs=[
                *[
                    pl.BlockSpec(
                        (1, lats, lon), functools.partial(lambda f, i, s: (f, 0, 0), 2 * pair + half)
                    )
                    for pair in pairs
                    for half in range(2)
                ],
                pl.BlockSpec((tile, lon), lambda i, s: (i, 0)),
                pl.BlockSpec((tile, 1), lambda i, s: (i, 0)),
                pl.BlockSpec((1, wide), lambda i, s: (0, 0)),
            ],
            out_specs=pl.BlockSpec((per, rows // dests, wide), lambda i, s: (i, 0, 0)),
            scratch_shapes=[pltpu.VMEM((wide, lon), BF)],
        ),
        out_shape=jax.ShapeDtypeStruct((dests, rows // dests, wide), BF),
        compiler_params=pltpu.CompilerParams(vmem_limit_bytes=VMEM_BYTES),
        cost_estimate=pl.CostEstimate(
            flops=2 * rows * wide * lon, bytes_accessed=2 * wide * (lon + rows), transcendentals=0
        ),
        name="dft",
    )(starts, *[grid_in] * count, angles, wave_row, jnp.tile(modes, (1, len(pairs))))


def inverse_kernel(starts, back, angles, wave_row, modes, *refs):
    out, turned = refs[-2:]
    first, second, rest = (pl.multiple_of(starts[i], HALF) for i in range(3))

    @pl.when(pl.program_id(1) == 0)
    def _():
        dests, rows, width = back.shape
        per = 8
        count = per * rows
        for i in range(dests // per):
            value = back[i * per : (i + 1) * per].reshape(count, width).astype(F32)
            value = jnp.where(wave_row[i * count : (i + 1) * count, :] < modes[...], value, 0.0)
            turned[:, i * count : (i + 1) * count] = (2.0 * value).astype(BF).T

    value = dot(turned[...], angles[...])
    for i in range(2):
        out[i, pl.ds(first, 128), :] = value[i * 256 : i * 256 + 128]
        out[i, pl.ds(second, 128), :] = value[i * 256 + 128 : i * 256 + 256]
        out[i, pl.ds(rest, HALF), :] = value[512 + i * HALF : 512 + (i + 1) * HALF]


def inverse_dft(back, angles, wave_row, modes, starts, shape, whole, pair):
    dests, rows, wide = back.shape
    _, lats, lon = shape
    width = 2 * lats
    pairs = wide // width
    step = lon // 3
    given = [] if whole is None else [whole]
    return pl.pallas_call(
        inverse_kernel,
        grid_spec=pltpu.PrefetchScalarGridSpec(
            num_scalar_prefetch=1,
            grid=(pairs, lon // step),
            in_specs=[
                pl.BlockSpec((dests, rows, width), lambda k, n, s: (0, 0, k)),
                pl.BlockSpec((dests * rows, step), lambda k, n, s: (0, n)),
                pl.BlockSpec((dests * rows, 1), lambda k, n, s: (0, 0)),
                pl.BlockSpec((1, width), lambda k, n, s: (0, 0)),
                *[pl.BlockSpec(memory_space=pl.ANY) for _ in given],
            ],
            out_specs=pl.BlockSpec((2, lats, step), lambda k, n, s: (pair + k, 0, n)),
            scratch_shapes=[pltpu.VMEM((width, dests * rows), BF)],
        ),
        out_shape=jax.ShapeDtypeStruct(shape, F32),
        input_output_aliases={5: 0} if given else {},
        compiler_params=pltpu.CompilerParams(vmem_limit_bytes=VMEM_BYTES),
        cost_estimate=pl.CostEstimate(
            flops=2 * dests * rows * wide * lon,
            bytes_accessed=wide * (4 * lon + 2 * dests * rows),
            transcendentals=0,
        ),
        name="inverse_dft",
    )(starts, back, angles, wave_row, modes, *given)


def legendre_kernel(
    lat_count,
    fld_count,
    lats,
    half_cols,
    pairs,
    arrived,
    low,
    h0,
    h1,
    h2,
    h3,
    degree4,
    rates,
    weights,
    gather,
    scatter,
    mirror,
    spectra,
    leaving,
    even,
    odd,
    north,
    south,
):
    pair = pl.program_id(1)
    blocks = lat_count // 2
    width = 2 * lats
    slot_rows = 2 * fld_count * pairs
    lower = lax.broadcasted_iota(jnp.int32, (GROUP * slot_rows, LANES), 1) < HALF
    flip_tile = mirror[0]
    flip_half = mirror[1]

    def swap(x):
        return pltpu.roll(x, HALF, 1)

    def put(ref, half, at, x):
        ref[:, half * slot_rows : (half + 1) * slot_rows, at : at + LANES] = x.astype(BF).reshape(
            GROUP, slot_rows, LANES
        )

    def get(ref, half, at):
        return ref[:, half * slot_rows : (half + 1) * slot_rows, at : at + LANES].reshape(
            GROUP * slot_rows, LANES
        )

    def stacked(lat):
        parts = [
            arrived[lat * fld_count + f, :, k * width : (k + 1) * width]
            for f in range(fld_count)
            for k in range(pairs)
        ]
        return dot(gather[...], jnp.concatenate(parts, 0))

    @pl.when(pair == 0)
    def _():
        rests = []
        for block in range(blocks):
            up = stacked(block)
            down = stacked(lat_count - 1 - block).astype(BF)
            for piece in range(5):
                tile = slice(piece * LANES, (piece + 1) * LANES)
                n = up[:, tile]
                s = dot(down[:, tile], flip_tile if piece < 4 else flip_half)
                w = weights[block : block + 1, 2 * LANES :] if piece == 4 else (
                    weights[block : block + 1, (piece % 2) * LANES : (piece % 2 + 1) * LANES]
                )
                e, o = (n + s) * w, (n - s) * w
                if piece < 4:
                    at = block * 256 + (piece % 2) * LANES
                    put(even, piece // 2, at, e)
                    put(odd, piece // 2, at, o)
                else:
                    rests.append((e, o))
        for b in range(blocks // 2):
            at = blocks * 256 + b * LANES
            for ref, c in ((even, 0), (odd, 1)):
                x, y = rests[2 * b][c], rests[2 * b + 1][c]
                put(ref, 0, at, jnp.where(lower, x, swap(y)))
                put(ref, 1, at, jnp.where(lower, swap(x), y))

    def rows_of(load):
        parts = [load(b * lats, 256) for b in range(blocks)]
        parts.append(jnp.concatenate([load(b * lats + 256, HALF) for b in range(blocks)], 0))
        return parts

    def transform(slot, local, even_table, odd_table, cols):
        def project(ref, parts):
            total = None
            for i, part in enumerate(parts):
                term = dot(ref[slot, :, i * 256 : i * 256 + part.shape[0]], part)
                total = term if total is None else total + term
            return total

        results = []
        tables = []
        for c, (ref, load) in enumerate(((even, even_table), (odd, odd_table))):
            parts = rows_of(load)
            tables.append(parts)
            d4 = degree4[local, :, c * half_cols : c * half_cols + cols]
            factor = jnp.where(d4 >= 0.0, 1.0 / (1.0 + rates[...] * d4), 0.0)
            results.append(project(ref, parts) * factor)
        for c, value in enumerate(results):
            for f in range(fld_count):
                for r in range(2):
                    at = (f * 2 + r) * pairs
                    both = jnp.concatenate(
                        [
                            value[half * slot_rows + at + k : half * slot_rows + at + k + 1]
                            for k in range(pairs)
                            for half in range(2)
                        ],
                        0,
                    )
                    spectra[f, r, local, :, c * half_cols : c * half_cols + cols] = both
                    if cols < half_cols:
                        spectra[f, r, local, :, c * half_cols + cols : (c + 1) * half_cols] = (
                            jnp.zeros((2 * pairs, half_cols - cols), F32)
                        )
        coeff = [v.astype(BF) for v in results]
        for i in range(blocks + 1):
            sym = dot_t(coeff[0], tables[0][i])
            anti = dot_t(coeff[1], tables[1][i])
            at = slice(i * 256, i * 256 + sym.shape[1])
            north[slot, :, at] = (sym + anti).astype(BF)
            south[slot, :, at] = (sym - anti).astype(BF)

    transform(
        2 * pair,
        0,
        lambda at, n: low[0, at : at + n, :half_cols],
        lambda at, n: low[0, at : at + n, half_cols:],
        half_cols,
    )
    transform(
        2 * pair + 1,
        1,
        lambda at, n: jnp.concatenate([h0[0, at : at + n, :], h1[0, at : at + n, :]], 1),
        lambda at, n: jnp.concatenate([h2[0, at : at + n, :], h3[0, at : at + n, :]], 1),
        2 * LANES,
    )

    @pl.when(pair == pl.num_programs(1) - 1)
    def _():
        for block in range(blocks):
            for ref, lat in ((north, block), (south, lat_count - 1 - block)):
                pieces = [
                    get(ref, half, block * 256 + t * LANES) for half in range(2) for t in range(2)
                ]
                at = blocks * 256 + (block // 2) * LANES
                x, y = get(ref, 0, at).astype(F32), get(ref, 1, at).astype(F32)
                rest = jnp.where(lower, x, swap(y)) if block % 2 == 0 else jnp.where(lower, swap(x), y)
                pieces.append(rest.astype(BF))
                if ref is south:
                    pieces = [
                        dot(p, flip_tile if i < 4 else flip_half).astype(BF)
                        for i, p in enumerate(pieces)
                    ]
                joined = dot(scatter[...], jnp.concatenate(pieces, 1)).astype(BF)
                for f in range(fld_count):
                    for k in range(pairs):
                        row = (f * pairs + k) * 2 * GROUP
                        leaving[lat * fld_count + f, :, k * width : (k + 1) * width] = joined[
                            row : row + 2 * GROUP
                        ]


def legendre_step(
    arrived, position, pairs, tables, own_waves, damp_rates, gauss_weight, lat_count, fld_count
):
    slots, half_lats, columns = tables.shape
    half_cols = columns // 2
    sources, travel_rows, _ = arrived.shape
    lats = 2 * half_lats // lat_count
    wide = 2 * lats * pairs
    slot_rows = 2 * fld_count * pairs
    rows = 2 * slot_rows
    blocks = lat_count // 2
    groups, inner = slots // GROUP, GROUP // 2

    col_index = jnp.arange(columns, dtype=jnp.int32)
    offset = jnp.where(col_index < half_cols, 2 * col_index, 2 * col_index - columns + 1)
    degree = own_waves[:, None] + offset[None, :]
    ratio = (degree * (degree + 1)).astype(F32) / float(LMAX * (LMAX + 1))
    degree4 = jnp.where(degree <= LMAX, ratio**4, -1.0)[:, None, :]

    rates = jnp.broadcast_to(
        damp_rates.transpose(2, 0, 1)[:, :, None, :], (2, fld_count, 2, pairs)
    ).reshape(rows, 1)
    w = gauss_weight.reshape(blocks, lats)
    weights = jnp.concatenate([w, w[:, 256:]], 1)

    size = GROUP * slot_rows
    target = jnp.arange(size, dtype=jnp.int32)
    s, rest = target // slot_rows, target % slot_rows
    f, rest = rest // (2 * pairs), rest % (2 * pairs)
    r, k = rest // pairs, rest % pairs
    source = ((f * pairs + k) * GROUP + s) * 2 + r
    gather = (source[:, None] == target[None, :]).astype(BF)
    scatter = (source[None, :] == target[:, None]).astype(BF)
    lane = jnp.arange(LANES, dtype=jnp.int32)
    place = lane[:, None] + lane[None, :]
    same_half = lane[:, None] // HALF == lane[None, :] // HALF
    mirror = jnp.stack(
        [place == LANES - 1, same_half & (place % LANES == HALF - 1)]
    ).astype(BF)

    def slot_of(g, p):
        return g * GROUP + 2 * p

    narrow = [
        pl.BlockSpec((1, half_lats, LANES), functools.partial(lambda t, g, p: (slot_of(g, p) + 1, 0, t), t))
        for t in (0, 1, half_cols // LANES, half_cols // LANES + 1)
    ]
    whole = lambda *shape: pl.BlockSpec(shape, lambda g, p: (0,) * len(shape))
    scratch = pltpu.VMEM((GROUP, rows, half_lats), BF)
    flops = 2 * 2 * slots * rows * half_lats * columns
    return pl.pallas_call(
        functools.partial(legendre_kernel, lat_count, fld_count, lats, half_cols, pairs),
        grid=(groups, inner),
        in_specs=[
            pl.BlockSpec((sources, 2 * GROUP, wide), lambda g, p: (0, g, position // pairs)),
            pl.BlockSpec((1, half_lats, columns), lambda g, p: (slot_of(g, p), 0, 0)),
            *narrow,
            pl.BlockSpec((2, 1, columns), lambda g, p: (g * inner + p, 0, 0)),
            whole(rows, 1),
            whole(blocks, 3 * LANES),
            whole(size, size),
            whole(size, size),
            whole(2, LANES, LANES),
        ],
        out_specs=[
            pl.BlockSpec(
                (fld_count, 2, 2, 2 * pairs, columns), lambda g, p: (0, 0, g * inner + p, 0, 0)
            ),
            pl.BlockSpec((sources, 2 * GROUP, wide), lambda g, p: (0, g, 0)),
        ],
        out_shape=[
            jax.ShapeDtypeStruct((fld_count, 2, slots, 2 * pairs, columns), F32),
            jax.ShapeDtypeStruct((sources, travel_rows, wide), BF),
        ],
        scratch_shapes=[scratch] * 4,
        compiler_params=pltpu.CompilerParams(vmem_limit_bytes=VMEM_BYTES),
        cost_estimate=pl.CostEstimate(
            flops=flops, bytes_accessed=2 * slots * half_lats * columns, transcendentals=0
        ),
        name="legendre",
    )(arrived, tables, *[tables] * 4, degree4, rates, weights, gather, scatter, mirror)


def fast_body(grid_in, legendre, wave_slot, lat_modes, gauss_weight, diffusion):
    fields, lats, lon = grid_in.shape
    slots_all = wave_slot.shape[0]
    lat_count = lax.axis_size("lat")
    fld_count = lax.axis_size("fld")
    owners = lat_count * fld_count
    owned = slots_all // owners
    lat_index = lax.axis_index("lat")
    owner = lat_index * fld_count + lax.axis_index("fld")
    southern = lat_index >= lat_count // 2
    starts = jnp.where(southern, jnp.array([192, 64, 0]), jnp.array([0, 128, 256])).astype(jnp.int32)
    flipped = jnp.concatenate([lat_modes[192:], lat_modes[64:192], lat_modes[:64]])
    ordered = jnp.where(southern, flipped, lat_modes)
    modes = jnp.concatenate([ordered[:256], ordered[:256], ordered[256:], ordered[256:]])[None, :]
    wave_row = jnp.repeat(wave_slot, 2)[:, None]
    own_waves = lax.dynamic_slice_in_dim(wave_slot, owner * owned, owned)
    rates = diffusion.reshape(fld_count, fields // 2, 2)

    def exchange(x):
        return lax.all_to_all(x, ("lat", "fld"), 0, 0, tiled=True)

    angles = angle_rows(wave_row, lon)
    arrived = [
        exchange(dft(grid_in, angles, wave_row, modes, starts, owners, pairs)) for pairs in OUTWARD
    ]
    parts, back = [], []
    for i, pairs in enumerate(RETURN):
        pair, count = pairs[0], len(pairs)
        source = next(j for j, out in enumerate(OUTWARD) if pair in out)
        values = arrived[source]
        if i >= 2:
            values, back[i - 2] = lax.optimization_barrier((values, back[i - 2]))
        part, leaving = legendre_step(
            values,
            OUTWARD[source].index(pair),
            count,
            legendre,
            own_waves,
            rates[:, pair : pair + count],
            gauss_weight,
            lat_count,
            fld_count,
        )
        parts.append(share_spectra(part))
        for waiting in parts[i - 1 : i + 1] if i == len(RETURN) - 1 else parts[i - 1 : i]:
            blocks = [block for _, block in waiting]
            leaving, blocks = lax.optimization_barrier((leaving, blocks))
            waiting[:] = [(at, block) for (at, _), block in zip(waiting, blocks)]
        back.append(exchange(leaving))
    whole = None
    columns = legendre.shape[2]
    spectra = jnp.zeros((2, fld_count, owned, fields, columns), F32)
    for i, pairs in enumerate(RETURN):
        if i == len(RETURN) - 1:
            whole, spectra = lax.optimization_barrier((whole, spectra))
            spectra = assemble(spectra, parts)
            back[i], spectra = lax.optimization_barrier((back[i], spectra))
        whole = inverse_dft(back[i], angles, wave_row, modes, starts, grid_in.shape, whole, pairs[0])
    return (whole, spectra.reshape(2, -1, fields, columns))


def assemble(spectra, parts):
    for pairs, blocks in zip(RETURN, parts):
        for at, block in blocks:
            spectra = lax.dynamic_update_slice(spectra, block[:, None], (0, at, 0, 2 * pairs[0], 0))
    return spectra


def share_spectra(part):
    count = part.shape[0]
    mine = lax.axis_index("fld")
    blocks = []
    for shift in range(count):
        block = lax.dynamic_index_in_dim(part, (mine + shift) % count, 0, keepdims=False)
        if shift:
            ring = [(i, (i + shift) % count) for i in range(count)]
            block = lax.ppermute(block, "fld", ring)
        blocks.append(((mine + count - shift) % count, block))
    return blocks


def angle_table(waves, lon_count):
    points = jnp.arange(lon_count, dtype=jnp.int32)
    phase_index = points[:, None] * waves[None, :] % lon_count
    radians = phase_index.astype(jnp.float32) * (2.0 * math.pi / lon_count)
    norm_scale = 1.0 / math.sqrt(lon_count)
    return jnp.stack([jnp.cos(radians) * norm_scale, -jnp.sin(radians) * norm_scale], 1).astype(
        jnp.bfloat16
    )


def damping(waves, damp_rates, columns):
    half_cols = columns // 2
    col_index = jnp.arange(columns, dtype=jnp.int32)
    offset = jnp.where(col_index < half_cols, 2 * col_index, 2 * col_index - columns + 1)
    degree = waves[:, None] + offset[None, :]
    degree_ratio = (degree * (degree + 1)).astype(jnp.float32) / float(LMAX * (LMAX + 1))
    factor = 1.0 / (1.0 + damp_rates[None, :, None] * (degree_ratio**4)[:, None, :])
    return jnp.where((degree <= LMAX)[:, None, :], factor, 0.0)


def project(even_part, odd_part, tables, used_cols):
    half_cols = tables.shape[2] // 2
    even_cols = jnp.einsum(
        "rsfj,sjq->rsfq", even_part, tables[:, :, :used_cols], preferred_element_type=jnp.float32
    )
    odd_cols = jnp.einsum(
        "rsfj,sjq->rsfq",
        odd_part,
        tables[:, :, half_cols : half_cols + used_cols],
        preferred_element_type=jnp.float32,
    )
    return jnp.concatenate([even_cols, odd_cols], -1)


def expand(rounded, tables, used_cols):
    half_cols = tables.shape[2] // 2
    sym_part = jnp.einsum(
        "rsfq,sjq->rsfj",
        rounded[..., :used_cols],
        tables[:, :, :used_cols],
        preferred_element_type=jnp.float32,
    )
    anti_part = jnp.einsum(
        "rsfq,sjq->rsfj",
        rounded[..., half_cols : half_cols + used_cols],
        tables[:, :, half_cols : half_cols + used_cols],
        preferred_element_type=jnp.float32,
    )
    return (sym_part, anti_part)


def transform_block(block_data, tables, block_waves, damp_rates, weights):
    half_lats = weights.shape[0]
    columns = tables.shape[2]
    half_cols = columns // 2
    north_half = block_data[..., :half_lats].astype(jnp.float32)
    south_half = jnp.flip(block_data[..., half_lats:], -1).astype(jnp.float32)
    even_part = ((north_half + south_half) * weights).astype(jnp.bfloat16)
    odd_part = ((north_half - south_half) * weights).astype(jnp.bfloat16)
    raw_coeff = project(even_part, odd_part, tables, half_cols)
    spectra = raw_coeff * damping(block_waves, damp_rates, columns)[None]
    rounded = spectra.astype(jnp.bfloat16)
    sym_part, anti_part = expand(rounded, tables, half_cols)
    synthesized = jnp.concatenate(
        [
            (sym_part + anti_part).astype(jnp.bfloat16),
            jnp.flip((sym_part - anti_part).astype(jnp.bfloat16), -1),
        ],
        -1,
    )
    return (spectra, synthesized)


def general_body(grid_in, legendre, wave_slot, lat_modes, gauss_weight, diffusion):
    fld_dev, lat_dev, lon_count = grid_in.shape
    slots_all = wave_slot.shape[0]
    lat_count = lax.axis_size("lat")
    fld_count = lax.axis_size("fld")
    lat_total = lat_dev * lat_count
    lat_index = lax.axis_index("lat")
    fld_index = lax.axis_index("fld")
    owned_slots = slots_all // (lat_count * fld_count)
    angles = angle_table(wave_slot, lon_count)
    keep_mask = (wave_slot[:, None] < lat_modes[None, :]).astype(jnp.float32)
    fourier = jnp.einsum("fjx,xrs->rsfj", grid_in, angles, preferred_element_type=jnp.float32)
    fourier = (fourier * keep_mask[None, :, None, :]).astype(jnp.bfloat16)
    own_waves = lax.dynamic_slice_in_dim(
        wave_slot, (lat_index * fld_count + fld_index) * owned_slots, owned_slots
    )
    flattened = fourier.reshape(2, slots_all, fld_dev * lat_dev)
    arrived = lax.all_to_all(flattened, ("lat", "fld"), split_axis=1, concat_axis=2, tiled=True)
    arrived = arrived.reshape(2, owned_slots, lat_count, fld_count, fld_dev, lat_dev)
    arrived = arrived.transpose(0, 1, 3, 4, 2, 5).reshape(
        2, owned_slots, fld_count * fld_dev, lat_total
    )
    owned_spectra, synthesized = transform_block(
        arrived, legendre, own_waves, diffusion, gauss_weight
    )
    spectra = lax.all_to_all(owned_spectra, "fld", split_axis=2, concat_axis=1, tiled=True)
    outgoing = synthesized.reshape(2, owned_slots, fld_count, fld_dev, lat_count, lat_dev)
    outgoing = outgoing.transpose(0, 1, 4, 2, 3, 5).reshape(
        2, owned_slots, lat_count * fld_count * fld_dev * lat_dev
    )
    returned = lax.all_to_all(outgoing, ("lat", "fld"), split_axis=2, concat_axis=1, tiled=True)
    returned = returned.reshape(2, slots_all, fld_dev, lat_dev)
    keep_narrow = keep_mask.astype(jnp.bfloat16)
    masked = returned * keep_narrow[None, :, None, :]
    grid_out = 2.0 * jnp.einsum("rsfj,xrs->fjx", masked, angles, preferred_element_type=jnp.float32)
    return (grid_out, spectra)


def body(grid_in, legendre, wave_slot, lat_modes, gauss_weight, diffusion):
    fields, lats, lon = grid_in.shape
    slots, _, columns = legendre.shape
    lat_count = lax.axis_size("lat")
    fits = (
        lats == 2 * LANES + HALF
        and lat_count % 4 == 0
        and fields == 2 * sum(map(len, OUTWARD))
        and lat_count * lax.axis_size("fld") % 8 == 0
        and slots % GROUP == 0
        and lon % (3 * LANES) == 0
        and columns == 6 * LANES
    )
    chosen = fast_body if fits else general_body
    return chosen(grid_in, legendre, wave_slot, lat_modes, gauss_weight, diffusion)


def solution(mesh):
    return jax.shard_map(
        body,
        mesh=mesh,
        in_specs=(P("fld", "lat", None), P(("lat", "fld"), None, None), P(), P("lat"), P(), P()),
        out_specs=(P("fld", "lat", None), P(None, "lat", "fld", None)),
        check_vma=False,
    )
```

```python
import functools
import math

import jax
import jax.numpy as jnp
from jax import lax
from jax.experimental import pallas as pl
from jax.experimental.pallas import tpu as pltpu
from jax.sharding import PartitionSpec as P

LMAX = 1279
LANES = 128
HALF = 64
GROUP = 8
OUTWARD = ((2,), (0, 1, 3))
RETURN = ((2,), (0, 1), (3,))
BF = jnp.bfloat16
F32 = jnp.float32
VMEM_BYTES = 66_000_000


def dot(a, b):
    return jnp.dot(a, b, preferred_element_type=F32)


def dot_t(a, b):
    return lax.dot_general(a, b, (((1,), (1,)), ((), ())), preferred_element_type=F32)


def turn_cos(phase, count):
    whole = phase - jnp.floor(phase * (1.0 / count) + 0.5) * count
    half = whole * (math.pi / count)
    square = half * half
    total = jnp.full_like(square, -1.0 / math.factorial(14))
    for order in range(12, -1, -2):
        total = total * square + (-1.0) ** (order // 2) / math.factorial(order)
    return 2.0 * (total * total) - 1.0


def angle_kernel(lon, wave_row, out):
    rows = out.shape[0]
    step = 128
    scale = 1.0 / math.sqrt(lon)
    tiles = lon // LANES
    middle = tiles // 2

    @pl.loop(0, rows // step)
    def _(i):
        at = pl.ds(pl.multiple_of(i * step, step), step)
        wave = jnp.broadcast_to(wave_row[at, :].astype(F32), (step, LANES))
        lane = lax.broadcasted_iota(jnp.int32, (step, LANES), 1).astype(F32)
        part = lax.broadcasted_iota(jnp.int32, (step, LANES), 0)
        turn = (part % 2 * (lon // 4)).astype(F32)
        fine = wave * lane + turn
        coarse = wave * LANES
        double = 2.0 * turn_cos(coarse, lon)
        pair = [turn_cos(fine + coarse * a, lon) * scale for a in (middle, middle + 1)]

        def put(a, x):
            out[at, a * LANES : (a + 1) * LANES] = x.astype(BF)

        put(middle, pair[0])
        put(middle + 1, pair[1])
        before, value = pair
        for a in range(middle + 2, tiles):
            before, value = value, double * value - before
            put(a, value)
        value, before = pair
        for a in range(middle - 1, -1, -1):
            before, value = value, double * value - before
            put(a, value)


def dft_kernel(count, makes_angles, starts, *refs):
    fields = refs[:count]
    if makes_angles:
        wave_row, modes, out, angles, arranged = refs[count:]
        angle_kernel(arranged.shape[1], wave_row, angles)
    else:
        wave_row, modes, angles, out, arranged = refs[count:]
    width = out.shape[2] // (count // 2)

    @pl.when(pl.program_id(0) == 0)
    def _():
        first, second, rest = (pl.multiple_of(starts[i], HALF) for i in range(3))
        for i, field in enumerate(fields):
            pair, half = divmod(i, 2)
            at = pair * width + half * 256
            arranged[at : at + 128] = field[0, pl.ds(first, 128), :]
            arranged[at + 128 : at + 256] = field[0, pl.ds(second, 128), :]
            at = pair * width + 512 + half * HALF
            arranged[at : at + HALF] = field[0, pl.ds(rest, HALF), :]

    value = dot_t(angles[...], arranged[...])
    value = jnp.where(wave_row[...] < modes[...], value, 0.0)
    out[...] = value.astype(BF).reshape(out.shape)


def dft(grid_in, angles, wave_row, modes, starts, dests, pairs):
    _, lats, lon = grid_in.shape
    count = 2 * len(pairs)
    rows = wave_row.shape[0]
    wide = count * lats
    per = dests // 4
    tile = rows * per // dests
    makes_angles = angles is None
    angle_spec = pl.BlockSpec((tile, lon), lambda i, s: (i, 0))
    out_spec = pl.BlockSpec((per, rows // dests, wide), lambda i, s: (i, 0, 0))
    out_shape = jax.ShapeDtypeStruct((dests, rows // dests, wide), BF)
    return pl.pallas_call(
        functools.partial(dft_kernel, count, makes_angles),
        grid_spec=pltpu.PrefetchScalarGridSpec(
            num_scalar_prefetch=1,
            grid=(dests // per,),
            in_specs=[
                *[
                    pl.BlockSpec(
                        (1, lats, lon), functools.partial(lambda f, i, s: (f, 0, 0), 2 * pair + half)
                    )
                    for pair in pairs
                    for half in range(2)
                ],
                pl.BlockSpec((tile, 1), lambda i, s: (i, 0)),
                pl.BlockSpec((1, wide), lambda i, s: (0, 0)),
                *([] if makes_angles else [angle_spec]),
            ],
            out_specs=[out_spec, angle_spec] if makes_angles else out_spec,
            scratch_shapes=[pltpu.VMEM((wide, lon), BF)],
        ),
        out_shape=[out_shape, jax.ShapeDtypeStruct((rows, lon), BF)] if makes_angles else out_shape,
        compiler_params=pltpu.CompilerParams(vmem_limit_bytes=VMEM_BYTES),
        cost_estimate=pl.CostEstimate(
            flops=2 * rows * wide * lon, bytes_accessed=2 * wide * (lon + rows), transcendentals=0
        ),
        name="dft",
    )(
        starts,
        *[grid_in] * count,
        wave_row,
        jnp.tile(modes, (1, len(pairs))),
        *([] if makes_angles else [angles]),
    )


def inverse_kernel(starts, back, angles, wave_row, modes, *refs):
    out, turned = refs[-2:]
    first, second, rest = (pl.multiple_of(starts[i], HALF) for i in range(3))

    @pl.when(pl.program_id(1) == 0)
    def _():
        dests, rows, width = back.shape
        per = 8
        count = per * rows
        for i in range(dests // per):
            value = back[i * per : (i + 1) * per].reshape(count, width).astype(F32)
            value = jnp.where(wave_row[i * count : (i + 1) * count, :] < modes[...], value, 0.0)
            turned[:, i * count : (i + 1) * count] = (2.0 * value).astype(BF).T

    value = dot(turned[...], angles[...])
    for i in range(2):
        out[i, pl.ds(first, 128), :] = value[i * 256 : i * 256 + 128]
        out[i, pl.ds(second, 128), :] = value[i * 256 + 128 : i * 256 + 256]
        out[i, pl.ds(rest, HALF), :] = value[512 + i * HALF : 512 + (i + 1) * HALF]


def inverse_dft(back, angles, wave_row, modes, starts, shape, whole, pair):
    dests, rows, wide = back.shape
    _, lats, lon = shape
    width = 2 * lats
    pairs = wide // width
    step = lon // 3
    given = [] if whole is None else [whole]
    return pl.pallas_call(
        inverse_kernel,
        grid_spec=pltpu.PrefetchScalarGridSpec(
            num_scalar_prefetch=1,
            grid=(pairs, lon // step),
            in_specs=[
                pl.BlockSpec((dests, rows, width), lambda k, n, s: (0, 0, k)),
                pl.BlockSpec((dests * rows, step), lambda k, n, s: (0, n)),
                pl.BlockSpec((dests * rows, 1), lambda k, n, s: (0, 0)),
                pl.BlockSpec((1, width), lambda k, n, s: (0, 0)),
                *[pl.BlockSpec(memory_space=pl.ANY) for _ in given],
            ],
            out_specs=pl.BlockSpec((2, lats, step), lambda k, n, s: (pair + k, 0, n)),
            scratch_shapes=[pltpu.VMEM((width, dests * rows), BF)],
        ),
        out_shape=jax.ShapeDtypeStruct(shape, F32),
        input_output_aliases={5: 0} if given else {},
        compiler_params=pltpu.CompilerParams(vmem_limit_bytes=VMEM_BYTES),
        cost_estimate=pl.CostEstimate(
            flops=2 * dests * rows * wide * lon,
            bytes_accessed=wide * (4 * lon + 2 * dests * rows),
            transcendentals=0,
        ),
        name="inverse_dft",
    )(starts, back, angles, wave_row, modes, *given)


def legendre_kernel(
    lat_count,
    fld_count,
    lats,
    half_cols,
    pairs,
    arrived,
    low,
    h0,
    h1,
    h2,
    h3,
    degree4,
    rates,
    weights,
    gather,
    scatter,
    mirror,
    spectra,
    leaving,
    even,
    odd,
    north,
    south,
):
    pair = pl.program_id(1)
    blocks = lat_count // 2
    width = 2 * lats
    slot_rows = 2 * fld_count * pairs
    lower = lax.broadcasted_iota(jnp.int32, (GROUP * slot_rows, LANES), 1) < HALF
    flip_tile = mirror[0]
    flip_half = mirror[1]

    def swap(x):
        return pltpu.roll(x, HALF, 1)

    def put(ref, half, at, x):
        ref[:, half * slot_rows : (half + 1) * slot_rows, at : at + LANES] = x.astype(BF).reshape(
            GROUP, slot_rows, LANES
        )

    def get(ref, half, at):
        return ref[:, half * slot_rows : (half + 1) * slot_rows, at : at + LANES].reshape(
            GROUP * slot_rows, LANES
        )

    def stacked(lat):
        parts = [
            arrived[lat * fld_count + f, :, k * width : (k + 1) * width]
            for f in range(fld_count)
            for k in range(pairs)
        ]
        return dot(gather[...], jnp.concatenate(parts, 0))

    @pl.when(pair == 0)
    def _():
        rests = []
        for block in range(blocks):
            up = stacked(block)
            down = stacked(lat_count - 1 - block).astype(BF)
            for piece in range(5):
                tile = slice(piece * LANES, (piece + 1) * LANES)
                n = up[:, tile]
                s = dot(down[:, tile], flip_tile if piece < 4 else flip_half)
                w = weights[block : block + 1, 2 * LANES :] if piece == 4 else (
                    weights[block : block + 1, (piece % 2) * LANES : (piece % 2 + 1) * LANES]
                )
                e, o = (n + s) * w, (n - s) * w
                if piece < 4:
                    at = block * 256 + (piece % 2) * LANES
                    put(even, piece // 2, at, e)
                    put(odd, piece // 2, at, o)
                else:
                    rests.append((e, o))
        for b in range(blocks // 2):
            at = blocks * 256 + b * LANES
            for ref, c in ((even, 0), (odd, 1)):
                x, y = rests[2 * b][c], rests[2 * b + 1][c]
                put(ref, 0, at, jnp.where(lower, x, swap(y)))
                put(ref, 1, at, jnp.where(lower, swap(x), y))

    def rows_of(load):
        parts = [load(b * lats, 256) for b in range(blocks)]
        parts.append(jnp.concatenate([load(b * lats + 256, HALF) for b in range(blocks)], 0))
        return parts

    def transform(slot, local, even_table, odd_table, cols):
        def project(ref, parts):
            total = None
            for i, part in enumerate(parts):
                term = dot(ref[slot, :, i * 256 : i * 256 + part.shape[0]], part)
                total = term if total is None else total + term
            return total

        results = []
        tables = []
        for c, (ref, load) in enumerate(((even, even_table), (odd, odd_table))):
            parts = rows_of(load)
            tables.append(parts)
            d4 = degree4[local, :, c * half_cols : c * half_cols + cols]
            factor = jnp.where(d4 >= 0.0, 1.0 / (1.0 + rates[...] * d4), 0.0)
            results.append(project(ref, parts) * factor)
        for c, value in enumerate(results):
            for f in range(fld_count):
                for r in range(2):
                    at = (f * 2 + r) * pairs
                    both = jnp.concatenate(
                        [
                            value[half * slot_rows + at + k : half * slot_rows + at + k + 1]
                            for k in range(pairs)
                            for half in range(2)
                        ],
                        0,
                    )
                    spectra[f, r, local, :, c * half_cols : c * half_cols + cols] = both
                    if cols < half_cols:
                        spectra[f, r, local, :, c * half_cols + cols : (c + 1) * half_cols] = (
                            jnp.zeros((2 * pairs, half_cols - cols), F32)
                        )
        coeff = [v.astype(BF) for v in results]
        for i in range(blocks + 1):
            sym = dot_t(coeff[0], tables[0][i])
            anti = dot_t(coeff[1], tables[1][i])
            at = slice(i * 256, i * 256 + sym.shape[1])
            north[slot, :, at] = (sym + anti).astype(BF)
            south[slot, :, at] = (sym - anti).astype(BF)

    transform(
        2 * pair,
        0,
        lambda at, n: low[0, at : at + n, :half_cols],
        lambda at, n: low[0, at : at + n, half_cols:],
        half_cols,
    )
    transform(
        2 * pair + 1,
        1,
        lambda at, n: jnp.concatenate([h0[0, at : at + n, :], h1[0, at : at + n, :]], 1),
        lambda at, n: jnp.concatenate([h2[0, at : at + n, :], h3[0, at : at + n, :]], 1),
        2 * LANES,
    )

    @pl.when(pair == pl.num_programs(1) - 1)
    def _():
        for block in range(blocks):
            for ref, lat in ((north, block), (south, lat_count - 1 - block)):
                pieces = [
                    get(ref, half, block * 256 + t * LANES) for half in range(2) for t in range(2)
                ]
                at = blocks * 256 + (block // 2) * LANES
                x, y = get(ref, 0, at).astype(F32), get(ref, 1, at).astype(F32)
                rest = jnp.where(lower, x, swap(y)) if block % 2 == 0 else jnp.where(lower, swap(x), y)
                pieces.append(rest.astype(BF))
                if ref is south:
                    pieces = [
                        dot(p, flip_tile if i < 4 else flip_half).astype(BF)
                        for i, p in enumerate(pieces)
                    ]
                joined = dot(scatter[...], jnp.concatenate(pieces, 1)).astype(BF)
                for f in range(fld_count):
                    for k in range(pairs):
                        row = (f * pairs + k) * 2 * GROUP
                        leaving[lat * fld_count + f, :, k * width : (k + 1) * width] = joined[
                            row : row + 2 * GROUP
                        ]


def legendre_step(
    arrived, position, pairs, tables, own_waves, damp_rates, gauss_weight, lat_count, fld_count
):
    slots, half_lats, columns = tables.shape
    half_cols = columns // 2
    sources, travel_rows, _ = arrived.shape
    lats = 2 * half_lats // lat_count
    wide = 2 * lats * pairs
    slot_rows = 2 * fld_count * pairs
    rows = 2 * slot_rows
    blocks = lat_count // 2
    groups, inner = slots // GROUP, GROUP // 2

    col_index = jnp.arange(columns, dtype=jnp.int32)
    offset = jnp.where(col_index < half_cols, 2 * col_index, 2 * col_index - columns + 1)
    degree = own_waves[:, None] + offset[None, :]
    ratio = (degree * (degree + 1)).astype(F32) / float(LMAX * (LMAX + 1))
    degree4 = jnp.where(degree <= LMAX, ratio**4, -1.0)[:, None, :]

    rates = jnp.broadcast_to(
        damp_rates.transpose(2, 0, 1)[:, :, None, :], (2, fld_count, 2, pairs)
    ).reshape(rows, 1)
    w = gauss_weight.reshape(blocks, lats)
    weights = jnp.concatenate([w, w[:, 256:]], 1)

    size = GROUP * slot_rows
    target = jnp.arange(size, dtype=jnp.int32)
    s, rest = target // slot_rows, target % slot_rows
    f, rest = rest // (2 * pairs), rest % (2 * pairs)
    r, k = rest // pairs, rest % pairs
    source = ((f * pairs + k) * GROUP + s) * 2 + r
    gather = (source[:, None] == target[None, :]).astype(BF)
    scatter = (source[None, :] == target[:, None]).astype(BF)
    lane = jnp.arange(LANES, dtype=jnp.int32)
    place = lane[:, None] + lane[None, :]
    same_half = lane[:, None] // HALF == lane[None, :] // HALF
    mirror = jnp.stack(
        [place == LANES - 1, same_half & (place % LANES == HALF - 1)]
    ).astype(BF)

    def slot_of(g, p):
        return g * GROUP + 2 * p

    narrow = [
        pl.BlockSpec((1, half_lats, LANES), functools.partial(lambda t, g, p: (slot_of(g, p) + 1, 0, t), t))
        for t in (0, 1, half_cols // LANES, half_cols // LANES + 1)
    ]
    whole = lambda *shape: pl.BlockSpec(shape, lambda g, p: (0,) * len(shape))
    scratch = pltpu.VMEM((GROUP, rows, half_lats), BF)
    flops = 2 * 2 * slots * rows * half_lats * columns
    return pl.pallas_call(
        functools.partial(legendre_kernel, lat_count, fld_count, lats, half_cols, pairs),
        grid=(groups, inner),
        in_specs=[
            pl.BlockSpec((sources, 2 * GROUP, wide), lambda g, p: (0, g, position // pairs)),
            pl.BlockSpec((1, half_lats, columns), lambda g, p: (slot_of(g, p), 0, 0)),
            *narrow,
            pl.BlockSpec((2, 1, columns), lambda g, p: (g * inner + p, 0, 0)),
            whole(rows, 1),
            whole(blocks, 3 * LANES),
            whole(size, size),
            whole(size, size),
            whole(2, LANES, LANES),
        ],
        out_specs=[
            pl.BlockSpec(
                (fld_count, 2, 2, 2 * pairs, columns), lambda g, p: (0, 0, g * inner + p, 0, 0)
            ),
            pl.BlockSpec((sources, 2 * GROUP, wide), lambda g, p: (0, g, 0)),
        ],
        out_shape=[
            jax.ShapeDtypeStruct((fld_count, 2, slots, 2 * pairs, columns), F32),
            jax.ShapeDtypeStruct((sources, travel_rows, wide), BF),
        ],
        scratch_shapes=[scratch] * 4,
        compiler_params=pltpu.CompilerParams(vmem_limit_bytes=VMEM_BYTES),
        cost_estimate=pl.CostEstimate(
            flops=flops, bytes_accessed=2 * slots * half_lats * columns, transcendentals=0
        ),
        name="legendre",
    )(arrived, tables, *[tables] * 4, degree4, rates, weights, gather, scatter, mirror)


def fast_body(grid_in, legendre, wave_slot, lat_modes, gauss_weight, diffusion):
    fields, lats, lon = grid_in.shape
    slots_all = wave_slot.shape[0]
    lat_count = lax.axis_size("lat")
    fld_count = lax.axis_size("fld")
    owners = lat_count * fld_count
    owned = slots_all // owners
    lat_index = lax.axis_index("lat")
    owner = lat_index * fld_count + lax.axis_index("fld")
    southern = lat_index >= lat_count // 2
    starts = jnp.where(southern, jnp.array([192, 64, 0]), jnp.array([0, 128, 256])).astype(jnp.int32)
    flipped = jnp.concatenate([lat_modes[192:], lat_modes[64:192], lat_modes[:64]])
    ordered = jnp.where(southern, flipped, lat_modes)
    modes = jnp.concatenate([ordered[:256], ordered[:256], ordered[256:], ordered[256:]])[None, :]
    wave_row = jnp.repeat(wave_slot, 2)[:, None]
    own_waves = lax.dynamic_slice_in_dim(wave_slot, owner * owned, owned)
    rates = diffusion.reshape(fld_count, fields // 2, 2)

    def exchange(x):
        return lax.all_to_all(x, ("lat", "fld"), 0, 0, tiled=True)

    sent, angles = dft(grid_in, None, wave_row, modes, starts, owners, OUTWARD[0])
    arrived = [exchange(sent)]
    for pairs in OUTWARD[1:]:
        arrived.append(exchange(dft(grid_in, angles, wave_row, modes, starts, owners, pairs)))
    parts, back = [], []
    for i, pairs in enumerate(RETURN):
        pair, count = pairs[0], len(pairs)
        source = next(j for j, out in enumerate(OUTWARD) if pair in out)
        values = arrived[source]
        if i >= 2:
            values, back[i - 2] = lax.optimization_barrier((values, back[i - 2]))
        part, leaving = legendre_step(
            values,
            OUTWARD[source].index(pair),
            count,
            legendre,
            own_waves,
            rates[:, pair : pair + count],
            gauss_weight,
            lat_count,
            fld_count,
        )
        parts.append(share_spectra(part))
        for waiting in parts[i - 1 : i + 1] if i == len(RETURN) - 1 else parts[i - 1 : i]:
            blocks = [block for _, block in waiting]
            leaving, blocks = lax.optimization_barrier((leaving, blocks))
            waiting[:] = [(at, block) for (at, _), block in zip(waiting, blocks)]
        back.append(exchange(leaving))
    whole = None
    columns = legendre.shape[2]
    spectra = jnp.zeros((2, fld_count, owned, fields, columns), F32)
    for i, pairs in enumerate(RETURN):
        if i == len(RETURN) - 1:
            whole, spectra = lax.optimization_barrier((whole, spectra))
            spectra = assemble(spectra, parts)
            back[i], spectra = lax.optimization_barrier((back[i], spectra))
        whole = inverse_dft(back[i], angles, wave_row, modes, starts, grid_in.shape, whole, pairs[0])
    return (whole, spectra.reshape(2, -1, fields, columns))


def assemble(spectra, parts):
    for pairs, blocks in zip(RETURN, parts):
        for at, block in blocks:
            spectra = lax.dynamic_update_slice(spectra, block[:, None], (0, at, 0, 2 * pairs[0], 0))
    return spectra


def share_spectra(part):
    count = part.shape[0]
    mine = lax.axis_index("fld")
    blocks = []
    for shift in range(count):
        block = lax.dynamic_index_in_dim(part, (mine + shift) % count, 0, keepdims=False)
        if shift:
            ring = [(i, (i + shift) % count) for i in range(count)]
            block = lax.ppermute(block, "fld", ring)
        blocks.append(((mine + count - shift) % count, block))
    return blocks


def angle_table(waves, lon_count):
    points = jnp.arange(lon_count, dtype=jnp.int32)
    phase_index = points[:, None] * waves[None, :] % lon_count
    radians = phase_index.astype(jnp.float32) * (2.0 * math.pi / lon_count)
    norm_scale = 1.0 / math.sqrt(lon_count)
    return jnp.stack([jnp.cos(radians) * norm_scale, -jnp.sin(radians) * norm_scale], 1).astype(
        jnp.bfloat16
    )


def damping(waves, damp_rates, columns):
    half_cols = columns // 2
    col_index = jnp.arange(columns, dtype=jnp.int32)
    offset = jnp.where(col_index < half_cols, 2 * col_index, 2 * col_index - columns + 1)
    degree = waves[:, None] + offset[None, :]
    degree_ratio = (degree * (degree + 1)).astype(jnp.float32) / float(LMAX * (LMAX + 1))
    factor = 1.0 / (1.0 + damp_rates[None, :, None] * (degree_ratio**4)[:, None, :])
    return jnp.where((degree <= LMAX)[:, None, :], factor, 0.0)


def project(even_part, odd_part, tables, used_cols):
    half_cols = tables.shape[2] // 2
    even_cols = jnp.einsum(
        "rsfj,sjq->rsfq", even_part, tables[:, :, :used_cols], preferred_element_type=jnp.float32
    )
    odd_cols = jnp.einsum(
        "rsfj,sjq->rsfq",
        odd_part,
        tables[:, :, half_cols : half_cols + used_cols],
        preferred_element_type=jnp.float32,
    )
    return jnp.concatenate([even_cols, odd_cols], -1)


def expand(rounded, tables, used_cols):
    half_cols = tables.shape[2] // 2
    sym_part = jnp.einsum(
        "rsfq,sjq->rsfj",
        rounded[..., :used_cols],
        tables[:, :, :used_cols],
        preferred_element_type=jnp.float32,
    )
    anti_part = jnp.einsum(
        "rsfq,sjq->rsfj",
        rounded[..., half_cols : half_cols + used_cols],
        tables[:, :, half_cols : half_cols + used_cols],
        preferred_element_type=jnp.float32,
    )
    return (sym_part, anti_part)


def transform_block(block_data, tables, block_waves, damp_rates, weights):
    half_lats = weights.shape[0]
    columns = tables.shape[2]
    half_cols = columns // 2
    north_half = block_data[..., :half_lats].astype(jnp.float32)
    south_half = jnp.flip(block_data[..., half_lats:], -1).astype(jnp.float32)
    even_part = ((north_half + south_half) * weights).astype(jnp.bfloat16)
    odd_part = ((north_half - south_half) * weights).astype(jnp.bfloat16)
    raw_coeff = project(even_part, odd_part, tables, half_cols)
    spectra = raw_coeff * damping(block_waves, damp_rates, columns)[None]
    rounded = spectra.astype(jnp.bfloat16)
    sym_part, anti_part = expand(rounded, tables, half_cols)
    synthesized = jnp.concatenate(
        [
            (sym_part + anti_part).astype(jnp.bfloat16),
            jnp.flip((sym_part - anti_part).astype(jnp.bfloat16), -1),
        ],
        -1,
    )
    return (spectra, synthesized)


def general_body(grid_in, legendre, wave_slot, lat_modes, gauss_weight, diffusion):
    fld_dev, lat_dev, lon_count = grid_in.shape
    slots_all = wave_slot.shape[0]
    lat_count = lax.axis_size("lat")
    fld_count = lax.axis_size("fld")
    lat_total = lat_dev * lat_count
    lat_index = lax.axis_index("lat")
    fld_index = lax.axis_index("fld")
    owned_slots = slots_all // (lat_count * fld_count)
    angles = angle_table(wave_slot, lon_count)
    keep_mask = (wave_slot[:, None] < lat_modes[None, :]).astype(jnp.float32)
    fourier = jnp.einsum("fjx,xrs->rsfj", grid_in, angles, preferred_element_type=jnp.float32)
    fourier = (fourier * keep_mask[None, :, None, :]).astype(jnp.bfloat16)
    own_waves = lax.dynamic_slice_in_dim(
        wave_slot, (lat_index * fld_count + fld_index) * owned_slots, owned_slots
    )
    flattened = fourier.reshape(2, slots_all, fld_dev * lat_dev)
    arrived = lax.all_to_all(flattened, ("lat", "fld"), split_axis=1, concat_axis=2, tiled=True)
    arrived = arrived.reshape(2, owned_slots, lat_count, fld_count, fld_dev, lat_dev)
    arrived = arrived.transpose(0, 1, 3, 4, 2, 5).reshape(
        2, owned_slots, fld_count * fld_dev, lat_total
    )
    owned_spectra, synthesized = transform_block(
        arrived, legendre, own_waves, diffusion, gauss_weight
    )
    spectra = lax.all_to_all(owned_spectra, "fld", split_axis=2, concat_axis=1, tiled=True)
    outgoing = synthesized.reshape(2, owned_slots, fld_count, fld_dev, lat_count, lat_dev)
    outgoing = outgoing.transpose(0, 1, 4, 2, 3, 5).reshape(
        2, owned_slots, lat_count * fld_count * fld_dev * lat_dev
    )
    returned = lax.all_to_all(outgoing, ("lat", "fld"), split_axis=2, concat_axis=1, tiled=True)
    returned = returned.reshape(2, slots_all, fld_dev, lat_dev)
    keep_narrow = keep_mask.astype(jnp.bfloat16)
    masked = returned * keep_narrow[None, :, None, :]
    grid_out = 2.0 * jnp.einsum("rsfj,xrs->fjx", masked, angles, preferred_element_type=jnp.float32)
    return (grid_out, spectra)


def body(grid_in, legendre, wave_slot, lat_modes, gauss_weight, diffusion):
    fields, lats, lon = grid_in.shape
    slots, _, columns = legendre.shape
    lat_count = lax.axis_size("lat")
    fits = (
        lats == 2 * LANES + HALF
        and lat_count % 4 == 0
        and fields == 2 * sum(map(len, OUTWARD))
        and lat_count * lax.axis_size("fld") % 8 == 0
        and slots % GROUP == 0
        and lon % (3 * LANES) == 0
        and columns == 6 * LANES
    )
    chosen = fast_body if fits else general_body
    return chosen(grid_in, legendre, wave_slot, lat_modes, gauss_weight, diffusion)


def solution(mesh):
    return jax.shard_map(
        body,
        mesh=mesh,
        in_specs=(P("fld", "lat", None), P(("lat", "fld"), None, None), P(), P("lat"), P(), P()),
        out_specs=(P("fld", "lat", None), P(None, "lat", "fld", None)),
        check_vma=False,
    )
```

```python
import functools
import math

import jax
import jax.numpy as jnp
from jax import lax
from jax.experimental import pallas as pl
from jax.experimental.pallas import tpu as pltpu
from jax.sharding import PartitionSpec as P

LMAX = 1279
LANES = 128
HALF = 64
GROUP = 8
OUTWARD = ((2,), (0, 1, 3))
RETURN = ((2,), (0, 1), (3,))
BF = jnp.bfloat16
F32 = jnp.float32
VMEM_BYTES = 66_000_000


def dot(a, b):
    return jnp.dot(a, b, preferred_element_type=F32)


def dot_t(a, b):
    return lax.dot_general(a, b, (((1,), (1,)), ((), ())), preferred_element_type=F32)


def turn_cos(phase, count):
    whole = phase - jnp.floor(phase * (1.0 / count) + 0.5) * count
    half = whole * (math.pi / count)
    square = half * half
    total = jnp.full_like(square, -1.0 / math.factorial(14))
    for order in range(12, -1, -2):
        total = total * square + (-1.0) ** (order // 2) / math.factorial(order)
    return 2.0 * (total * total) - 1.0


def angle_kernel(lon, wave_row, out):
    rows = out.shape[0]
    step = 128
    scale = 1.0 / math.sqrt(lon)
    tiles = lon // LANES
    middle = tiles // 2

    @pl.loop(0, rows // step)
    def _(i):
        at = pl.ds(pl.multiple_of(i * step, step), step)
        wave = jnp.broadcast_to(wave_row[at, :].astype(F32), (step, LANES))
        lane = lax.broadcasted_iota(jnp.int32, (step, LANES), 1).astype(F32)
        part = lax.broadcasted_iota(jnp.int32, (step, LANES), 0)
        turn = (part % 2 * (lon // 4)).astype(F32)
        fine = wave * lane + turn
        coarse = wave * LANES
        double = 2.0 * turn_cos(coarse, lon)
        pair = [turn_cos(fine + coarse * a, lon) * scale for a in (middle, middle + 1)]

        def put(a, x):
            out[at, a * LANES : (a + 1) * LANES] = x.astype(BF)

        put(middle, pair[0])
        put(middle + 1, pair[1])
        before, value = pair
        for a in range(middle + 2, tiles):
            before, value = value, double * value - before
            put(a, value)
        value, before = pair
        for a in range(middle - 1, -1, -1):
            before, value = value, double * value - before
            put(a, value)


def dft_kernel(count, makes_angles, starts, *refs):
    fields = refs[:count]
    if makes_angles:
        wave_row, modes, out, angles, arranged = refs[count:]
        angle_kernel(arranged.shape[1], wave_row, angles)
    else:
        wave_row, modes, angles, out, arranged = refs[count:]
    width = out.shape[2] // (count // 2)

    @pl.when(pl.program_id(0) == 0)
    def _():
        first, second, rest = (pl.multiple_of(starts[i], HALF) for i in range(3))
        for i, field in enumerate(fields):
            pair, half = divmod(i, 2)
            at = pair * width + half * 256
            arranged[at : at + 128] = field[0, pl.ds(first, 128), :]
            arranged[at + 128 : at + 256] = field[0, pl.ds(second, 128), :]
            at = pair * width + 512 + half * HALF
            arranged[at : at + HALF] = field[0, pl.ds(rest, HALF), :]

    value = dot_t(angles[...], arranged[...])
    value = jnp.where(wave_row[...] < modes[...], value, 0.0)
    out[...] = value.astype(BF).reshape(out.shape)


def dft(grid_in, angles, wave_row, modes, starts, dests, pairs):
    _, lats, lon = grid_in.shape
    count = 2 * len(pairs)
    rows = wave_row.shape[0]
    wide = count * lats
    per = dests // (2 if angles is None else 4)
    tile = rows * per // dests
    makes_angles = angles is None
    angle_spec = pl.BlockSpec((tile, lon), lambda i, s: (i, 0))
    out_spec = pl.BlockSpec((per, rows // dests, wide), lambda i, s: (i, 0, 0))
    out_shape = jax.ShapeDtypeStruct((dests, rows // dests, wide), BF)
    return pl.pallas_call(
        functools.partial(dft_kernel, count, makes_angles),
        grid_spec=pltpu.PrefetchScalarGridSpec(
            num_scalar_prefetch=1,
            grid=(dests // per,),
            in_specs=[
                *[
                    pl.BlockSpec(
                        (1, lats, lon), functools.partial(lambda f, i, s: (f, 0, 0), 2 * pair + half)
                    )
                    for pair in pairs
                    for half in range(2)
                ],
                pl.BlockSpec((tile, 1), lambda i, s: (i, 0)),
                pl.BlockSpec((1, wide), lambda i, s: (0, 0)),
                *([] if makes_angles else [angle_spec]),
            ],
            out_specs=[out_spec, angle_spec] if makes_angles else out_spec,
            scratch_shapes=[pltpu.VMEM((wide, lon), BF)],
        ),
        out_shape=[out_shape, jax.ShapeDtypeStruct((rows, lon), BF)] if makes_angles else out_shape,
        compiler_params=pltpu.CompilerParams(vmem_limit_bytes=VMEM_BYTES),
        cost_estimate=pl.CostEstimate(
            flops=2 * rows * wide * lon, bytes_accessed=2 * wide * (lon + rows), transcendentals=0
        ),
        name="dft",
    )(
        starts,
        *[grid_in] * count,
        wave_row,
        jnp.tile(modes, (1, len(pairs))),
        *([] if makes_angles else [angles]),
    )


def inverse_kernel(starts, back, angles, wave_row, modes, *refs):
    out, turned = refs[-2:]
    first, second, rest = (pl.multiple_of(starts[i], HALF) for i in range(3))

    @pl.when(pl.program_id(1) == 0)
    def _():
        dests, rows, width = back.shape
        per = 8
        count = per * rows
        for i in range(dests // per):
            value = back[i * per : (i + 1) * per].reshape(count, width).astype(F32)
            value = jnp.where(wave_row[i * count : (i + 1) * count, :] < modes[...], value, 0.0)
            turned[:, i * count : (i + 1) * count] = (2.0 * value).astype(BF).T

    value = dot(turned[...], angles[...])
    for i in range(2):
        out[i, pl.ds(first, 128), :] = value[i * 256 : i * 256 + 128]
        out[i, pl.ds(second, 128), :] = value[i * 256 + 128 : i * 256 + 256]
        out[i, pl.ds(rest, HALF), :] = value[512 + i * HALF : 512 + (i + 1) * HALF]


def inverse_dft(back, angles, wave_row, modes, starts, shape, whole, pair):
    dests, rows, wide = back.shape
    _, lats, lon = shape
    width = 2 * lats
    pairs = wide // width
    step = lon // 3
    given = [] if whole is None else [whole]
    return pl.pallas_call(
        inverse_kernel,
        grid_spec=pltpu.PrefetchScalarGridSpec(
            num_scalar_prefetch=1,
            grid=(pairs, lon // step),
            in_specs=[
                pl.BlockSpec((dests, rows, width), lambda k, n, s: (0, 0, k)),
                pl.BlockSpec((dests * rows, step), lambda k, n, s: (0, n)),
                pl.BlockSpec((dests * rows, 1), lambda k, n, s: (0, 0)),
                pl.BlockSpec((1, width), lambda k, n, s: (0, 0)),
                *[pl.BlockSpec(memory_space=pl.ANY) for _ in given],
            ],
            out_specs=pl.BlockSpec((2, lats, step), lambda k, n, s: (pair + k, 0, n)),
            scratch_shapes=[pltpu.VMEM((width, dests * rows), BF)],
        ),
        out_shape=jax.ShapeDtypeStruct(shape, F32),
        input_output_aliases={5: 0} if given else {},
        compiler_params=pltpu.CompilerParams(vmem_limit_bytes=VMEM_BYTES),
        cost_estimate=pl.CostEstimate(
            flops=2 * dests * rows * wide * lon,
            bytes_accessed=wide * (4 * lon + 2 * dests * rows),
            transcendentals=0,
        ),
        name="inverse_dft",
    )(starts, back, angles, wave_row, modes, *given)


def legendre_kernel(
    lat_count,
    fld_count,
    lats,
    half_cols,
    pairs,
    arrived,
    low,
    h0,
    h1,
    h2,
    h3,
    degree4,
    rates,
    weights,
    gather,
    scatter,
    mirror,
    spectra,
    leaving,
    even,
    odd,
    north,
    south,
):
    pair = pl.program_id(1)
    blocks = lat_count // 2
    width = 2 * lats
    slot_rows = 2 * fld_count * pairs
    lower = lax.broadcasted_iota(jnp.int32, (GROUP * slot_rows, LANES), 1) < HALF
    flip_tile = mirror[0]
    flip_half = mirror[1]

    def swap(x):
        return pltpu.roll(x, HALF, 1)

    def put(ref, half, at, x):
        ref[:, half * slot_rows : (half + 1) * slot_rows, at : at + LANES] = x.astype(BF).reshape(
            GROUP, slot_rows, LANES
        )

    def get(ref, half, at):
        return ref[:, half * slot_rows : (half + 1) * slot_rows, at : at + LANES].reshape(
            GROUP * slot_rows, LANES
        )

    def stacked(lat):
        parts = [
            arrived[lat * fld_count + f, :, k * width : (k + 1) * width]
            for f in range(fld_count)
            for k in range(pairs)
        ]
        return dot(gather[...], jnp.concatenate(parts, 0))

    @pl.when(pair == 0)
    def _():
        rests = []
        for block in range(blocks):
            up = stacked(block)
            down = stacked(lat_count - 1 - block).astype(BF)
            for piece in range(5):
                tile = slice(piece * LANES, (piece + 1) * LANES)
                n = up[:, tile]
                s = dot(down[:, tile], flip_tile if piece < 4 else flip_half)
                w = weights[block : block + 1, 2 * LANES :] if piece == 4 else (
                    weights[block : block + 1, (piece % 2) * LANES : (piece % 2 + 1) * LANES]
                )
                e, o = (n + s) * w, (n - s) * w
                if piece < 4:
                    at = block * 256 + (piece % 2) * LANES
                    put(even, piece // 2, at, e)
                    put(odd, piece // 2, at, o)
                else:
                    rests.append((e, o))
        for b in range(blocks // 2):
            at = blocks * 256 + b * LANES
            for ref, c in ((even, 0), (odd, 1)):
                x, y = rests[2 * b][c], rests[2 * b + 1][c]
                put(ref, 0, at, jnp.where(lower, x, swap(y)))
                put(ref, 1, at, jnp.where(lower, swap(x), y))

    def rows_of(load):
        parts = [load(b * lats, 256) for b in range(blocks)]
        parts.append(jnp.concatenate([load(b * lats + 256, HALF) for b in range(blocks)], 0))
        return parts

    def transform(slot, local, even_table, odd_table, cols):
        def project(ref, parts):
            total = None
            for i, part in enumerate(parts):
                term = dot(ref[slot, :, i * 256 : i * 256 + part.shape[0]], part)
                total = term if total is None else total + term
            return total

        results = []
        tables = []
        for c, (ref, load) in enumerate(((even, even_table), (odd, odd_table))):
            parts = rows_of(load)
            tables.append(parts)
            d4 = degree4[local, :, c * half_cols : c * half_cols + cols]
            factor = jnp.where(d4 >= 0.0, 1.0 / (1.0 + rates[...] * d4), 0.0)
            results.append(project(ref, parts) * factor)
        for c, value in enumerate(results):
            for f in range(fld_count):
                for r in range(2):
                    at = (f * 2 + r) * pairs
                    both = jnp.concatenate(
                        [
                            value[half * slot_rows + at + k : half * slot_rows + at + k + 1]
                            for k in range(pairs)
                            for half in range(2)
                        ],
                        0,
                    )
                    spectra[f, r, local, :, c * half_cols : c * half_cols + cols] = both
                    if cols < half_cols:
                        spectra[f, r, local, :, c * half_cols + cols : (c + 1) * half_cols] = (
                            jnp.zeros((2 * pairs, half_cols - cols), F32)
                        )
        coeff = [v.astype(BF) for v in results]
        for i in range(blocks + 1):
            sym = dot_t(coeff[0], tables[0][i])
            anti = dot_t(coeff[1], tables[1][i])
            at = slice(i * 256, i * 256 + sym.shape[1])
            north[slot, :, at] = (sym + anti).astype(BF)
            south[slot, :, at] = (sym - anti).astype(BF)

    transform(
        2 * pair,
        0,
        lambda at, n: low[0, at : at + n, :half_cols],
        lambda at, n: low[0, at : at + n, half_cols:],
        half_cols,
    )
    transform(
        2 * pair + 1,
        1,
        lambda at, n: jnp.concatenate([h0[0, at : at + n, :], h1[0, at : at + n, :]], 1),
        lambda at, n: jnp.concatenate([h2[0, at : at + n, :], h3[0, at : at + n, :]], 1),
        2 * LANES,
    )

    @pl.when(pair == pl.num_programs(1) - 1)
    def _():
        for block in range(blocks):
            for ref, lat in ((north, block), (south, lat_count - 1 - block)):
                pieces = [
                    get(ref, half, block * 256 + t * LANES) for half in range(2) for t in range(2)
                ]
                at = blocks * 256 + (block // 2) * LANES
                x, y = get(ref, 0, at).astype(F32), get(ref, 1, at).astype(F32)
                rest = jnp.where(lower, x, swap(y)) if block % 2 == 0 else jnp.where(lower, swap(x), y)
                pieces.append(rest.astype(BF))
                if ref is south:
                    pieces = [
                        dot(p, flip_tile if i < 4 else flip_half).astype(BF)
                        for i, p in enumerate(pieces)
                    ]
                joined = dot(scatter[...], jnp.concatenate(pieces, 1)).astype(BF)
                for f in range(fld_count):
                    for k in range(pairs):
                        row = (f * pairs + k) * 2 * GROUP
                        leaving[lat * fld_count + f, :, k * width : (k + 1) * width] = joined[
                            row : row + 2 * GROUP
                        ]


def legendre_step(
    arrived, position, pairs, tables, own_waves, damp_rates, gauss_weight, lat_count, fld_count
):
    slots, half_lats, columns = tables.shape
    half_cols = columns // 2
    sources, travel_rows, _ = arrived.shape
    lats = 2 * half_lats // lat_count
    wide = 2 * lats * pairs
    slot_rows = 2 * fld_count * pairs
    rows = 2 * slot_rows
    blocks = lat_count // 2
    groups, inner = slots // GROUP, GROUP // 2

    col_index = jnp.arange(columns, dtype=jnp.int32)
    offset = jnp.where(col_index < half_cols, 2 * col_index, 2 * col_index - columns + 1)
    degree = own_waves[:, None] + offset[None, :]
    ratio = (degree * (degree + 1)).astype(F32) / float(LMAX * (LMAX + 1))
    degree4 = jnp.where(degree <= LMAX, ratio**4, -1.0)[:, None, :]

    rates = jnp.broadcast_to(
        damp_rates.transpose(2, 0, 1)[:, :, None, :], (2, fld_count, 2, pairs)
    ).reshape(rows, 1)
    w = gauss_weight.reshape(blocks, lats)
    weights = jnp.concatenate([w, w[:, 256:]], 1)

    size = GROUP * slot_rows
    target = jnp.arange(size, dtype=jnp.int32)
    s, rest = target // slot_rows, target % slot_rows
    f, rest = rest // (2 * pairs), rest % (2 * pairs)
    r, k = rest // pairs, rest % pairs
    source = ((f * pairs + k) * GROUP + s) * 2 + r
    gather = (source[:, None] == target[None, :]).astype(BF)
    scatter = (source[None, :] == target[:, None]).astype(BF)
    lane = jnp.arange(LANES, dtype=jnp.int32)
    place = lane[:, None] + lane[None, :]
    same_half = lane[:, None] // HALF == lane[None, :] // HALF
    mirror = jnp.stack(
        [place == LANES - 1, same_half & (place % LANES == HALF - 1)]
    ).astype(BF)

    def slot_of(g, p):
        return g * GROUP + 2 * p

    narrow = [
        pl.BlockSpec((1, half_lats, LANES), functools.partial(lambda t, g, p: (slot_of(g, p) + 1, 0, t), t))
        for t in (0, 1, half_cols // LANES, half_cols // LANES + 1)
    ]
    whole = lambda *shape: pl.BlockSpec(shape, lambda g, p: (0,) * len(shape))
    scratch = pltpu.VMEM((GROUP, rows, half_lats), BF)
    flops = 2 * 2 * slots * rows * half_lats * columns
    return pl.pallas_call(
        functools.partial(legendre_kernel, lat_count, fld_count, lats, half_cols, pairs),
        grid=(groups, inner),
        in_specs=[
            pl.BlockSpec((sources, 2 * GROUP, wide), lambda g, p: (0, g, position // pairs)),
            pl.BlockSpec((1, half_lats, columns), lambda g, p: (slot_of(g, p), 0, 0)),
            *narrow,
            pl.BlockSpec((2, 1, columns), lambda g, p: (g * inner + p, 0, 0)),
            whole(rows, 1),
            whole(blocks, 3 * LANES),
            whole(size, size),
            whole(size, size),
            whole(2, LANES, LANES),
        ],
        out_specs=[
            pl.BlockSpec(
                (fld_count, 2, 2, 2 * pairs, columns), lambda g, p: (0, 0, g * inner + p, 0, 0)
            ),
            pl.BlockSpec((sources, 2 * GROUP, wide), lambda g, p: (0, g, 0)),
        ],
        out_shape=[
            jax.ShapeDtypeStruct((fld_count, 2, slots, 2 * pairs, columns), F32),
            jax.ShapeDtypeStruct((sources, travel_rows, wide), BF),
        ],
        scratch_shapes=[scratch] * 4,
        compiler_params=pltpu.CompilerParams(vmem_limit_bytes=VMEM_BYTES),
        cost_estimate=pl.CostEstimate(
            flops=flops, bytes_accessed=2 * slots * half_lats * columns, transcendentals=0
        ),
        name="legendre",
    )(arrived, tables, *[tables] * 4, degree4, rates, weights, gather, scatter, mirror)


def fast_body(grid_in, legendre, wave_slot, lat_modes, gauss_weight, diffusion):
    fields, lats, lon = grid_in.shape
    slots_all = wave_slot.shape[0]
    lat_count = lax.axis_size("lat")
    fld_count = lax.axis_size("fld")
    owners = lat_count * fld_count
    owned = slots_all // owners
    lat_index = lax.axis_index("lat")
    owner = lat_index * fld_count + lax.axis_index("fld")
    southern = lat_index >= lat_count // 2
    starts = jnp.where(southern, jnp.array([192, 64, 0]), jnp.array([0, 128, 256])).astype(jnp.int32)
    flipped = jnp.concatenate([lat_modes[192:], lat_modes[64:192], lat_modes[:64]])
    ordered = jnp.where(southern, flipped, lat_modes)
    modes = jnp.concatenate([ordered[:256], ordered[:256], ordered[256:], ordered[256:]])[None, :]
    wave_row = jnp.repeat(wave_slot, 2)[:, None]
    own_waves = lax.dynamic_slice_in_dim(wave_slot, owner * owned, owned)
    rates = diffusion.reshape(fld_count, fields // 2, 2)

    def exchange(x):
        return lax.all_to_all(x, ("lat", "fld"), 0, 0, tiled=True)

    sent, angles = dft(grid_in, None, wave_row, modes, starts, owners, OUTWARD[0])
    arrived = [exchange(sent)]
    for pairs in OUTWARD[1:]:
        arrived.append(exchange(dft(grid_in, angles, wave_row, modes, starts, owners, pairs)))
    parts, back = [], []
    for i, pairs in enumerate(RETURN):
        pair, count = pairs[0], len(pairs)
        source = next(j for j, out in enumerate(OUTWARD) if pair in out)
        values = arrived[source]
        if i >= 2:
            values, back[i - 2] = lax.optimization_barrier((values, back[i - 2]))
        part, leaving = legendre_step(
            values,
            OUTWARD[source].index(pair),
            count,
            legendre,
            own_waves,
            rates[:, pair : pair + count],
            gauss_weight,
            lat_count,
            fld_count,
        )
        parts.append(share_spectra(part))
        for waiting in parts[i - 1 : i + 1] if i == len(RETURN) - 1 else parts[i - 1 : i]:
            blocks = [block for _, block in waiting]
            leaving, blocks = lax.optimization_barrier((leaving, blocks))
            waiting[:] = [(at, block) for (at, _), block in zip(waiting, blocks)]
        back.append(exchange(leaving))
    whole = None
    columns = legendre.shape[2]
    spectra = jnp.zeros((2, fld_count, owned, fields, columns), F32)
    for i, pairs in enumerate(RETURN):
        if i == len(RETURN) - 1:
            whole, spectra = lax.optimization_barrier((whole, spectra))
            spectra = assemble(spectra, parts)
            back[i], spectra = lax.optimization_barrier((back[i], spectra))
        whole = inverse_dft(back[i], angles, wave_row, modes, starts, grid_in.shape, whole, pairs[0])
    return (whole, spectra.reshape(2, -1, fields, columns))


def assemble(spectra, parts):
    for pairs, blocks in zip(RETURN, parts):
        for at, block in blocks:
            spectra = lax.dynamic_update_slice(spectra, block[:, None], (0, at, 0, 2 * pairs[0], 0))
    return spectra


def share_spectra(part):
    count = part.shape[0]
    mine = lax.axis_index("fld")
    blocks = []
    for shift in range(count):
        block = lax.dynamic_index_in_dim(part, (mine + shift) % count, 0, keepdims=False)
        if shift:
            ring = [(i, (i + shift) % count) for i in range(count)]
            block = lax.ppermute(block, "fld", ring)
        blocks.append(((mine + count - shift) % count, block))
    return blocks


def angle_table(waves, lon_count):
    points = jnp.arange(lon_count, dtype=jnp.int32)
    phase_index = points[:, None] * waves[None, :] % lon_count
    radians = phase_index.astype(jnp.float32) * (2.0 * math.pi / lon_count)
    norm_scale = 1.0 / math.sqrt(lon_count)
    return jnp.stack([jnp.cos(radians) * norm_scale, -jnp.sin(radians) * norm_scale], 1).astype(
        jnp.bfloat16
    )


def damping(waves, damp_rates, columns):
    half_cols = columns // 2
    col_index = jnp.arange(columns, dtype=jnp.int32)
    offset = jnp.where(col_index < half_cols, 2 * col_index, 2 * col_index - columns + 1)
    degree = waves[:, None] + offset[None, :]
    degree_ratio = (degree * (degree + 1)).astype(jnp.float32) / float(LMAX * (LMAX + 1))
    factor = 1.0 / (1.0 + damp_rates[None, :, None] * (degree_ratio**4)[:, None, :])
    return jnp.where((degree <= LMAX)[:, None, :], factor, 0.0)


def project(even_part, odd_part, tables, used_cols):
    half_cols = tables.shape[2] // 2
    even_cols = jnp.einsum(
        "rsfj,sjq->rsfq", even_part, tables[:, :, :used_cols], preferred_element_type=jnp.float32
    )
    odd_cols = jnp.einsum(
        "rsfj,sjq->rsfq",
        odd_part,
        tables[:, :, half_cols : half_cols + used_cols],
        preferred_element_type=jnp.float32,
    )
    return jnp.concatenate([even_cols, odd_cols], -1)


def expand(rounded, tables, used_cols):
    half_cols = tables.shape[2] // 2
    sym_part = jnp.einsum(
        "rsfq,sjq->rsfj",
        rounded[..., :used_cols],
        tables[:, :, :used_cols],
        preferred_element_type=jnp.float32,
    )
    anti_part = jnp.einsum(
        "rsfq,sjq->rsfj",
        rounded[..., half_cols : half_cols + used_cols],
        tables[:, :, half_cols : half_cols + used_cols],
        preferred_element_type=jnp.float32,
    )
    return (sym_part, anti_part)


def transform_block(block_data, tables, block_waves, damp_rates, weights):
    half_lats = weights.shape[0]
    columns = tables.shape[2]
    half_cols = columns // 2
    north_half = block_data[..., :half_lats].astype(jnp.float32)
    south_half = jnp.flip(block_data[..., half_lats:], -1).astype(jnp.float32)
    even_part = ((north_half + south_half) * weights).astype(jnp.bfloat16)
    odd_part = ((north_half - south_half) * weights).astype(jnp.bfloat16)
    raw_coeff = project(even_part, odd_part, tables, half_cols)
    spectra = raw_coeff * damping(block_waves, damp_rates, columns)[None]
    rounded = spectra.astype(jnp.bfloat16)
    sym_part, anti_part = expand(rounded, tables, half_cols)
    synthesized = jnp.concatenate(
        [
            (sym_part + anti_part).astype(jnp.bfloat16),
            jnp.flip((sym_part - anti_part).astype(jnp.bfloat16), -1),
        ],
        -1,
    )
    return (spectra, synthesized)


def general_body(grid_in, legendre, wave_slot, lat_modes, gauss_weight, diffusion):
    fld_dev, lat_dev, lon_count = grid_in.shape
    slots_all = wave_slot.shape[0]
    lat_count = lax.axis_size("lat")
    fld_count = lax.axis_size("fld")
    lat_total = lat_dev * lat_count
    lat_index = lax.axis_index("lat")
    fld_index = lax.axis_index("fld")
    owned_slots = slots_all // (lat_count * fld_count)
    angles = angle_table(wave_slot, lon_count)
    keep_mask = (wave_slot[:, None] < lat_modes[None, :]).astype(jnp.float32)
    fourier = jnp.einsum("fjx,xrs->rsfj", grid_in, angles, preferred_element_type=jnp.float32)
    fourier = (fourier * keep_mask[None, :, None, :]).astype(jnp.bfloat16)
    own_waves = lax.dynamic_slice_in_dim(
        wave_slot, (lat_index * fld_count + fld_index) * owned_slots, owned_slots
    )
    flattened = fourier.reshape(2, slots_all, fld_dev * lat_dev)
    arrived = lax.all_to_all(flattened, ("lat", "fld"), split_axis=1, concat_axis=2, tiled=True)
    arrived = arrived.reshape(2, owned_slots, lat_count, fld_count, fld_dev, lat_dev)
    arrived = arrived.transpose(0, 1, 3, 4, 2, 5).reshape(
        2, owned_slots, fld_count * fld_dev, lat_total
    )
    owned_spectra, synthesized = transform_block(
        arrived, legendre, own_waves, diffusion, gauss_weight
    )
    spectra = lax.all_to_all(owned_spectra, "fld", split_axis=2, concat_axis=1, tiled=True)
    outgoing = synthesized.reshape(2, owned_slots, fld_count, fld_dev, lat_count, lat_dev)
    outgoing = outgoing.transpose(0, 1, 4, 2, 3, 5).reshape(
        2, owned_slots, lat_count * fld_count * fld_dev * lat_dev
    )
    returned = lax.all_to_all(outgoing, ("lat", "fld"), split_axis=2, concat_axis=1, tiled=True)
    returned = returned.reshape(2, slots_all, fld_dev, lat_dev)
    keep_narrow = keep_mask.astype(jnp.bfloat16)
    masked = returned * keep_narrow[None, :, None, :]
    grid_out = 2.0 * jnp.einsum("rsfj,xrs->fjx", masked, angles, preferred_element_type=jnp.float32)
    return (grid_out, spectra)


def body(grid_in, legendre, wave_slot, lat_modes, gauss_weight, diffusion):
    fields, lats, lon = grid_in.shape
    slots, _, columns = legendre.shape
    lat_count = lax.axis_size("lat")
    fits = (
        lats == 2 * LANES + HALF
        and lat_count % 4 == 0
        and fields == 2 * sum(map(len, OUTWARD))
        and lat_count * lax.axis_size("fld") % 8 == 0
        and slots % GROUP == 0
        and lon % (3 * LANES) == 0
        and columns == 6 * LANES
    )
    chosen = fast_body if fits else general_body
    return chosen(grid_in, legendre, wave_slot, lat_modes, gauss_weight, diffusion)


def solution(mesh):
    return jax.shard_map(
        body,
        mesh=mesh,
        in_specs=(P("fld", "lat", None), P(("lat", "fld"), None, None), P(), P("lat"), P(), P()),
        out_specs=(P("fld", "lat", None), P(None, "lat", "fld", None)),
        check_vma=False,
    )
```
